512 devices in a mesh: seq: 16 (over x_hi, y), res: 32 (over z, x_lo, core).
Axes of the slice: x: 4 (x_hi: 2, x_lo: 2; x = x_hi * 2 + x_lo), y: 8, z: 8, core: 2. Of those that a mesh axis runs over, the one named last changes fastest.
Arguments:
- alignment: float32 [1024, 256, 256], P('seq', 'res'), may hold values from -100 to 100
- pair_features: float32 [256, 256, 128], P('seq', 'res'), may hold values from -100 to 100
- outer_gain: float32 [256], replicated, may hold values from 0.5 to 1.5
- w_outer_in: float32 [256, 64], replicated, may hold values from -0.375 to 0.375
- w_outer_out: float32 [1024, 128], replicated, may hold values from -0.1875 to 0.1875
- pair_gain: float32 [128], replicated, may hold values from 0.5 to 1.5
- w_bias: float32 [128, 8], replicated, may hold values from -30 to 30
- row_gain: float32 [256], replicated, may hold values from 0.5 to 1.5
- w_project: float32 [256, 1024], replicated, may hold values from -0.375 to 0.375
- w_output: float32 [256, 256], replicated, may hold values from -0.375 to 0.375
Outputs:
- alignment_out: float32 [1024, 256, 256], P('seq', 'res')
- updated_pair_array: float32 [256, 256, 128], P('seq', 'res')
The draws below stay inside these ranges and needn't reach their ends.
All inputs are finite; a program needn't handle non-finite values.
Results may differ from the reference program's by a relative error of at most 0.00018.
Values sent between devices are 32-bit elements; how exact they have to be, the bound alone decides.
No kernel may reach another device: no remote copies, remote signals or barrier semaphores. Data moves between devices by JAX's collectives and lax.ppermute only.
A program may use at most 128 MiB of HBM per device.

```python
import math
import jax
import jax.numpy as jnp
from jax import lax

CM = 256
CZ = 128
C = 32
H = 8
SEQS = 1024
RES = 256
N_SEQ = 16


def draw_alignment(key, part):
    profile = jax.random.normal(jax.random.fold_in(key, 11), (1, RES, CM), jnp.float32)
    jitter = jax.random.normal(jax.random.fold_in(key, 12), (SEQS, RES, CM), jnp.float32)
    return profile + jitter


def draw_pair_features(key, part):
    jitter = jax.random.normal(jax.random.fold_in(key, 21), (RES, RES, CZ), jnp.float32)
    return jitter


def draw_w_bias(key, part):
    base_map = jax.random.normal(jax.random.fold_in(key, 31), (CZ, H), jnp.float32) / math.sqrt(CZ)
    return base_map


def normal_values(key, shape, width, limit, held_as=jnp.bfloat16):
    drawn = width * jax.random.normal(key, shape, jnp.float32)
    return jnp.clip(drawn, min=-limit, max=limit).astype(held_as)


def setup_inputs(seed: int = 0) -> dict:
    seeds = jax.random.split(jax.random.key(seed), 11)
    alignment = draw_alignment(jax.random.fold_in(seeds[10], 71), 0)
    pair_features = draw_pair_features(jax.random.fold_in(seeds[10], 71), 0)
    outer_gain = jnp.clip(1.0 + 0.1 * jax.random.normal(seeds[2], (CM,), jnp.float32), 0.5, 1.5)
    w_outer_in = normal_values(seeds[3], (CM, 2 * C), CM ** -0.5, 0.375, jnp.float32)
    w_outer_out = normal_values(seeds[4], (C * C, CZ), (C * C) ** -0.5, 0.1875, jnp.float32)
    pair_gain = jnp.clip(1.0 + 0.1 * jax.random.normal(seeds[5], (CZ,), jnp.float32), 0.5, 1.5)
    w_bias = draw_w_bias(jax.random.fold_in(seeds[10], 71), 0)
    row_gain = jnp.clip(1.0 + 0.1 * jax.random.normal(seeds[7], (CM,), jnp.float32), 0.5, 1.5)
    w_project = normal_values(seeds[8], (CM, 4 * CM), CM ** -0.5, 0.375, jnp.float32)
    w_output = normal_values(seeds[9], (CM, CM), CM ** -0.5, 0.375, jnp.float32)
    return {"alignment": alignment, "pair_features": pair_features, "outer_gain": outer_gain, "w_outer_in": w_outer_in, "w_outer_out": w_outer_out, "pair_gain": pair_gain, "w_bias": w_bias, "row_gain": row_gain, "w_project": w_project, "w_output": w_output}


precise = lax.Precision.HIGHEST

def layer_norm(values, scales):
    average = lax.optimization_barrier(jnp.mean(values, axis=-1, keepdims=True))
    centered = values - average
    variance = lax.optimization_barrier(jnp.mean(centered * centered, axis=-1, keepdims=True))
    return centered * lax.rsqrt(variance + 1e-05) * scales

def row_attention(sequence, bias_all, row_gain, w_project, w_output):
    residues, channels = sequence.shape
    head_count = bias_all.shape[0]
    head_size = channels // head_count
    normed_rows = layer_norm(sequence, row_gain)
    projected = jnp.dot(normed_rows, w_project, precision=precise, preferred_element_type=jnp.float32)
    query_map = projected[:, :channels].reshape(residues, head_count, head_size) * head_size ** (-0.5)
    key_map = projected[:, channels:2 * channels].reshape(residues, head_count, head_size)
    value_map = projected[:, 2 * channels:3 * channels].reshape(residues, head_count, head_size)
    gate_map = projected[:, 3 * channels:]
    scores = jnp.einsum('ihd,jhd->hij', query_map, key_map, precision=precise) + bias_all
    weights = jax.nn.softmax(scores, axis=-1)
    mixed_heads = jnp.einsum('hij,jhd->ihd', weights, value_map, precision=precise).reshape(residues, channels)
    gated_out = jax.nn.sigmoid(gate_map) * mixed_heads
    return sequence + jnp.dot(gated_out, w_output, precision=precise, preferred_element_type=jnp.float32)

def reference(alignment, pair_features, outer_gain, w_outer_in, w_outer_out, pair_gain, w_bias, row_gain, w_project, w_output):
    seq_total = alignment.shape[0]
    residues = alignment.shape[1]
    channels = w_outer_in.shape[1] // 2
    normed_rows = layer_norm(alignment, outer_gain)
    both_maps = jnp.einsum('src,cd->sdr', normed_rows, w_outer_in, precision=precise)
    left_maps = both_maps[:, :channels]
    right_maps = both_maps[:, channels:]
    row_block = residues // N_SEQ
    left_blocks = left_maps.reshape(seq_total, channels, N_SEQ, row_block).transpose(2, 0, 1, 3)

    def outer_block(left_part):
        summed = jnp.einsum('sxi,syj->ijxy', left_part, right_maps, precision=precise)
        mean_outer = (summed / seq_total).reshape(row_block, residues, channels * channels)
        return jnp.einsum('ijk,kc->ijc', mean_outer, w_outer_out, precision=precise)
    pair_update = lax.map(outer_block, left_blocks).reshape(residues, residues, w_outer_out.shape[1])
    updated_pair_array = pair_features + pair_update
    bias_all = jnp.einsum('ijc,ch->hij', layer_norm(updated_pair_array, pair_gain), w_bias, precision=precise)

    def attend_one(sequence):
        return row_attention(sequence, bias_all, row_gain, w_project, w_output)
    alignment_out = lax.map(attend_one, alignment)
    return (alignment_out, updated_pair_array)
```

```python
import functools

import jax
import jax.numpy as jnp
from jax import lax
from jax.experimental import pallas as pl
from jax.experimental.pallas import tpu as pltpu
from jax.sharding import Mesh, PartitionSpec as P

f32 = jnp.float32
bf16 = jnp.bfloat16
precise = lax.Precision.HIGHEST

SEQ = ("xh", "yh", "yl")
RES = ("zh", "zl", "xl", "core")
CUBE = ("zl", "xl", "core")


def dot6(a, b, dims=(((1,), (0,)), ((), ()))):
    return lax.dot_general(a, b, dims, precision=precise, preferred_element_type=f32)


def halves(x):
    high = x.astype(bf16)
    low = (x - high.astype(f32)).astype(bf16)
    return high, low


def dot_parts(a, b, dims=(((1,), (0,)), ((), ()))):
    dot = functools.partial(lax.dot_general, dimension_numbers=dims, preferred_element_type=f32)
    return dot(a[0], b[0]) + (dot(a[0], b[1]) + dot(a[1], b[0]))


def dot3(a, b, dims=(((1,), (0,)), ((), ()))):
    return dot_parts(halves(a), halves(b), dims)


def center_scale(x):
    average = jnp.mean(x, axis=-1, keepdims=True)
    centered = x - average
    variance = jnp.mean(centered * centered, axis=-1, keepdims=True)
    return centered * lax.rsqrt(variance + 1e-05)


def lane_group(shape):
    return lax.broadcasted_iota(jnp.int32, shape, len(shape) - 1) // 32


def lanes_moved(x, shift):
    rows = x.reshape(-1, 128)
    return pltpu.roll(rows, shift % 128, 1).reshape(x.shape)


def swap_groups(parts):
    group = lane_group(parts[0].shape)
    low = group % 2 == 0
    x = [None] * 4
    for a in (0, 2):
        x[a] = jnp.where(low, parts[a], lanes_moved(parts[a + 1], 32))
        x[a + 1] = jnp.where(low, lanes_moved(parts[a], -32), parts[a + 1])
    first = group < 2
    y = [None] * 4
    for a in (0, 1):
        y[a] = jnp.where(first, x[a], lanes_moved(x[a + 2], 64))
        y[a + 2] = jnp.where(first, lanes_moved(x[a], 64), x[a + 2])
    return y


def maps_kernel(rows_ref, gain_ref, weight_ref, left_ref, right_ref, maps_ref):
    weight = weight_ref[...] * gain_ref[...]
    maps_ref[...] = dot6(center_scale(rows_ref[...]), weight)
    count = left_ref.shape[1]
    group = lane_group((count, 128))
    for half in range(2):
        left = jnp.zeros((count, 128), f32)
        right = jnp.zeros((count, 128), f32)
        for k in range(4):
            part = maps_ref[pl.ds(half * 4 + k, count, stride=8), :]
            left = jnp.where(group == k, lanes_moved(part, 32 * k), left)
            right = jnp.where(group == k, lanes_moved(part, 32 * k - 32), right)
        for copy in range(2):
            left_ref[copy * 2 + half] = left
        for copy in range(8):
            right_ref[copy, :, half * 128 : half * 128 + 128] = right


def project_kernel(rows_ref, gain_ref, weight_ref, qkv_ref, gate_ref):
    weight = weight_ref[...] * gain_ref[...]
    normed = halves(center_scale(rows_ref[...]))
    for t in range(4):
        block = dot_parts(normed, halves(weight[:, t * 256 : t * 256 + 256]))
        if t == 3:
            gate_ref[...] = jax.nn.sigmoid(block)
            continue
        if t == 0:
            block = block * 32 ** (-0.5)
        for half in range(2):
            part = block[:, half * 128 : half * 128 + 128].reshape(16, 4, 8, 128)
            moved = swap_groups([part[:, s] for s in range(4)])
            for h in range(4):
                own = moved[h].reshape(4, 4, 8, 128)
                for n in range(4):
                    qkv_ref[half * 4 + h, t, n] = own[:, n]


def outer_kernel(left_ref, right_ref, weight_ref, out_ref, turned_ref, rows_ref):
    for r in range(4):
        both = jnp.concatenate([right_ref[r], right_ref[4 + r]], axis=0)
        turned_ref[r] = both.T
    for y in range(32):
        for r in range(4):
            rows_ref[(y * 4 + r) * 8 : (y * 4 + r) * 8 + 8, :] = turned_ref[r, pl.ds(y, 8, stride=32), :]

    def step(z, carry):
        left = jnp.concatenate([left_ref[z, 0], left_ref[z, 1]], axis=0)
        outer = dot6(rows_ref[...], left).reshape(8, 4, 32, 128)
        moved = swap_groups([outer[:, y] for y in range(4)])
        lhs = jnp.concatenate(
            [jnp.concatenate([moved[i][y] for y in range(8)], axis=1) for i in range(4)], axis=0
        )
        update = dot6(lhs, weight_ref[...]).reshape(4, 4, 8, 128)
        for r in range(4):
            out_ref[z, r] = update[:, r]
        return carry

    lax.fori_loop(0, 8, step, 0)


def pair_kernel(parts_ref, pair_ref, gain_ref, weight_ref, pair_out_ref, bias_ref):
    total = parts_ref[0]
    for g in range(1, 8):
        total = total + parts_ref[g]
    total = total * (1.0 / 1024.0)
    for x in range(2):
        for c in range(2):
            at = c * 8 + x * 4
            pair_out_ref[at : at + 4] = pair_ref[at : at + 4] + total[(x * 2 + c) * 4 : (x * 2 + c) * 4 + 4]
    normed = center_scale(pair_out_ref[...].reshape(128, 128)) * gain_ref[...]
    bias_ref[...] = dot6(weight_ref[...], normed, (((1,), (1,)), ((), ())))


def residues(ref, t, n):
    return jnp.concatenate([ref[:, t, n, z].reshape(64, 128) for z in range(4)], axis=0)


def attend_kernel(qkv_ref, bias_ref, out_ref):
    bias = bias_ref[...].reshape(256, 256)
    group = lane_group((256, 128))

    def step(n, carry):
        query = residues(qkv_ref, 0, n)
        key = halves(residues(qkv_ref, 1, n))
        value = halves(residues(qkv_ref, 2, n))
        mixed = jnp.zeros((256, 128), f32)
        for s in range(4):
            own = halves(jnp.where(group == s, query, 0.0))
            scores = dot_parts(own, key, (((1,), (1,)), ((), ()))) + bias
            top = jnp.max(scores, axis=-1, keepdims=True)
            weights = jnp.exp(scores - top)
            total = jnp.sum(weights, axis=-1, keepdims=True)
            mixed = jnp.where(group == s, dot_parts(halves(weights), value) / total, mixed)
        for z in range(4):
            out_ref[:, z, n] = mixed[z * 64 : z * 64 + 64].reshape(8, 8, 128)
        return carry

    lax.fori_loop(0, 4, step, 0)


def output_kernel(mixed_ref, gate_ref, rows_ref, weight_ref, out_ref):
    columns = []
    for half in range(2):
        parts = [mixed_ref[half * 4 + h].reshape(16, 8, 128) for h in range(4)]
        moved = swap_groups(parts)
        columns.append(jnp.stack(moved, axis=1).reshape(512, 128))
    gated = jnp.concatenate(columns, axis=1) * gate_ref[...]
    out_ref[...] = rows_ref[...] + dot3(gated, weight_ref[...])


def shape_of(*lengths):
    return jax.ShapeDtypeStruct(lengths, f32)


def call(kernel, name, flops, out_shape, *args, scratch=()):
    return pl.pallas_call(
        kernel,
        out_shape=out_shape,
        scratch_shapes=list(scratch),
        name=name,
        cost_estimate=pl.CostEstimate(flops=flops, bytes_accessed=2**20, transcendentals=0),
        compiler_params=pltpu.CompilerParams(vmem_limit_bytes=40 * 2**20),
    )(*args)


def exchanged(value, axes):
    return lax.all_to_all(value, axes, 0, 0, tiled=True)


def sent_to_all(value, axes):
    count = lax.axis_size(axes)
    return exchanged(jnp.broadcast_to(value[None], (count, *value.shape)), axes)


def on_device(
    alignment,
    pair_features,
    outer_gain,
    w_outer_in,
    w_outer_out,
    pair_gain,
    w_bias,
    row_gain,
    w_project,
    w_output,
):
    own_rows = alignment.reshape(512, 256)
    w_in = jnp.pad(w_outer_in, ((0, 0), (0, 64)))
    w_out = w_outer_out.reshape(32, 32, 128).transpose(1, 0, 2).reshape(1024, 128)
    left, right = call(
        maps_kernel,
        "maps",
        10**9,
        (shape_of(4, 64, 128), shape_of(8, 64, 256)),
        own_rows,
        outer_gain.reshape(256, 1),
        w_in,
        scratch=[pltpu.VMEM((512, 128), f32)],
    )
    rows = exchanged(alignment.reshape(4, 16, 8, 256), "zh").reshape(512, 256)
    left, rows = lax.optimization_barrier((left, rows))
    left = exchanged(left, ("yl", "xl")).reshape(2, 2, 64, 128)
    left = lax.dynamic_index_in_dim(left, lax.axis_index("yl"), axis=1, keepdims=False)
    left_all = sent_to_all(left, ("zh", "zl")).reshape(8, 2, 64, 128)
    right, left_all = lax.optimization_barrier((right, left_all))
    right_all = exchanged(right, ("yl", "xl", "core"))
    qkv, gate = call(
        project_kernel,
        "project",
        4 * 10**9,
        (shape_of(8, 3, 4, 4, 8, 128), shape_of(512, 256)),
        rows,
        row_gain.reshape(256, 1),
        w_project,
    )
    qkv, right_all = lax.optimization_barrier((qkv, right_all))
    qkv = exchanged(qkv, CUBE)
    parts = call(
        outer_kernel,
        "outer",
        4 * 10**9,
        shape_of(8, 4, 4, 8, 128),
        left_all,
        right_all,
        w_out,
        scratch=[pltpu.VMEM((4, 256, 128), f32), pltpu.VMEM((1024, 128), f32)],
    )
    parts, qkv = lax.optimization_barrier((parts, qkv))
    parts = exchanged(parts.reshape(32, 4, 8, 128), ("xh", "yh", "xl", "core"))
    updated_pair, bias = call(
        pair_kernel,
        "pair",
        10**8,
        (shape_of(16, 8, 128), shape_of(8, 128)),
        parts.reshape(8, 16, 8, 128),
        pair_features,
        pair_gain.reshape(1, 128),
        w_bias.T,
    )
    bias = exchanged(bias, CUBE)
    bias = sent_to_all(bias, "zh").reshape(32, 16, 8)
    bias = bias.transpose(1, 0, 2).reshape(16, 256)
    bias = sent_to_all(bias, SEQ).reshape(16, 16, 256)
    mixed = call(attend_kernel, "attend", 4 * 10**9, shape_of(8, 4, 4, 8, 128), qkv, bias)
    mixed = exchanged(mixed, CUBE)
    out = call(
        output_kernel,
        "output",
        10**9,
        shape_of(512, 256),
        mixed,
        gate,
        rows,
        w_output,
    )
    out = exchanged(out.reshape(4, 16, 8, 256), "zh")
    return out.reshape(alignment.shape), updated_pair


def solution(mesh):
    fine = Mesh(
        mesh.devices.reshape(2, 4, 2, 4, 2, 2, 2), ("xh", "yh", "yl", "zh", "zl", "xl", "core")
    )
    tiled = P(SEQ, RES, None)
    return jax.shard_map(
        on_device,
        mesh=fine,
        in_specs=(tiled, tiled) + (P(),) * 8,
        out_specs=(tiled, tiled),
        check_vma=False,
    )
```

```python
import functools

import jax
import jax.numpy as jnp
from jax import lax
from jax.experimental import pallas as pl
from jax.experimental.pallas import tpu as pltpu
from jax.sharding import Mesh, PartitionSpec as P

f32 = jnp.float32
bf16 = jnp.bfloat16
precise = lax.Precision.HIGHEST

SEQ = ("xh", "yh", "yl")
RES = ("zh", "zl", "xl", "core")
CUBE = ("zl", "xl", "core")


def dot6(a, b, dims=(((1,), (0,)), ((), ()))):
    return lax.dot_general(a, b, dims, precision=precise, preferred_element_type=f32)


def halves(x):
    high = x.astype(bf16)
    low = (x - high.astype(f32)).astype(bf16)
    return high, low


def dot_parts(a, b, dims=(((1,), (0,)), ((), ()))):
    dot = functools.partial(lax.dot_general, dimension_numbers=dims, preferred_element_type=f32)
    return dot(a[0], b[0]) + (dot(a[0], b[1]) + dot(a[1], b[0]))


def dot3(a, b, dims=(((1,), (0,)), ((), ()))):
    return dot_parts(halves(a), halves(b), dims)


def center_scale(x):
    average = jnp.mean(x, axis=-1, keepdims=True)
    centered = x - average
    variance = jnp.mean(centered * centered, axis=-1, keepdims=True)
    return centered * lax.rsqrt(variance + 1e-05)


def lane_group(shape):
    return lax.broadcasted_iota(jnp.int32, shape, len(shape) - 1) // 32


def lanes_moved(x, shift):
    rows = x.reshape(-1, 128)
    return pltpu.roll(rows, shift % 128, 1).reshape(x.shape)


def swap_groups(parts):
    group = lane_group(parts[0].shape)
    low = group % 2 == 0
    x = [None] * 4
    for a in (0, 2):
        x[a] = jnp.where(low, parts[a], lanes_moved(parts[a + 1], 32))
        x[a + 1] = jnp.where(low, lanes_moved(parts[a], -32), parts[a + 1])
    first = group < 2
    y = [None] * 4
    for a in (0, 1):
        y[a] = jnp.where(first, x[a], lanes_moved(x[a + 2], 64))
        y[a + 2] = jnp.where(first, lanes_moved(x[a], 64), x[a + 2])
    return y


def maps_kernel(rows_ref, gain_ref, weight_ref, left_ref, right_ref, maps_ref):
    weight = weight_ref[...] * gain_ref[...]
    maps_ref[...] = dot6(center_scale(rows_ref[...]), weight)
    count = left_ref.shape[1]
    group = lane_group((count, 128))
    for half in range(2):
        left = jnp.zeros((count, 128), f32)
        right = jnp.zeros((count, 128), f32)
        for k in range(4):
            part = maps_ref[pl.ds(half * 4 + k, count, stride=8), :]
            left = jnp.where(group == k, lanes_moved(part, 32 * k), left)
            right = jnp.where(group == k, lanes_moved(part, 32 * k - 32), right)
        left_ref[half] = left
        right_ref[:, half * 128 : half * 128 + 128] = right


def project_kernel(rows_ref, gain_ref, weight_ref, qkv_ref):
    weight = weight_ref[...] * gain_ref[...]
    normed = halves(center_scale(rows_ref[...]))
    for t in range(3):
        block = dot_parts(normed, halves(weight[:, t * 256 : t * 256 + 256]))
        if t == 0:
            block = block * 32 ** (-0.5)
        for half in range(2):
            part = block[:, half * 128 : half * 128 + 128].reshape(16, 4, 8, 128)
            moved = swap_groups([part[:, s] for s in range(4)])
            for h in range(4):
                own = moved[h].reshape(4, 4, 8, 128)
                for n in range(4):
                    qkv_ref[half * 4 + h, t, n] = own[:, n]


def gate_kernel(rows_ref, gain_ref, weight_ref, gate_ref):
    weight = weight_ref[:, 768:] * gain_ref[...]
    gate_ref[...] = jax.nn.sigmoid(dot3(center_scale(rows_ref[...]), weight))


def outer_kernel(left_ref, own_ref, other_ref, weight_ref, out_ref, turned_ref, rows_ref):
    for r in range(4):
        both = jnp.concatenate([own_ref[r], other_ref[r]], axis=0)
        turned_ref[r] = both.T
    for y in range(32):
        for r in range(4):
            rows_ref[(y * 4 + r) * 8 : (y * 4 + r) * 8 + 8, :] = turned_ref[r, pl.ds(y, 8, stride=32), :]

    def step(z, carry):
        left = jnp.concatenate([left_ref[z, 0], left_ref[z, 1]], axis=0)
        outer = dot6(rows_ref[...], left).reshape(8, 4, 32, 128)
        moved = swap_groups([outer[:, y] for y in range(4)])
        lhs = jnp.concatenate(
            [jnp.concatenate([moved[i][y] for y in range(8)], axis=1) for i in range(4)], axis=0
        )
        update = dot6(lhs, weight_ref[...]).reshape(4, 4, 8, 128)
        for r in range(4):
            out_ref[z // 4, r, z % 4] = update[:, r]
        return carry

    lax.fori_loop(0, 8, step, 0)


def add_kernel(parts_ref, out_ref):
    for y in range(4):
        out_ref[y] = parts_ref[0, :, y] + parts_ref[1, :, y]


def pair_kernel(parts_ref, pair_ref, gain_ref, weight_ref, pair_out_ref, bias_ref):
    total = parts_ref[0]
    for g in range(1, 4):
        total = total + parts_ref[g]
    total = total * (1.0 / 1024.0)
    for x in range(2):
        for c in range(2):
            at = c * 8 + x * 4
            pair_out_ref[at : at + 4] = pair_ref[at : at + 4] + total[(x * 2 + c) * 4 : (x * 2 + c) * 4 + 4]
    normed = center_scale(pair_out_ref[...].reshape(128, 128)) * gain_ref[...]
    bias_ref[...] = dot6(weight_ref[...], normed, (((1,), (1,)), ((), ())))


def residues(ref, t, n):
    return jnp.concatenate([ref[:, t, n, z].reshape(64, 128) for z in range(4)], axis=0)


def attend_kernel(qkv_ref, bias_ref, out_ref):
    bias = bias_ref[...].reshape(256, 256)
    group = lane_group((256, 128))

    def step(n, carry):
        query = residues(qkv_ref, 0, n)
        key = halves(residues(qkv_ref, 1, n))
        value = halves(residues(qkv_ref, 2, n))
        mixed = jnp.zeros((256, 128), f32)
        for s in range(4):
            own = halves(jnp.where(group == s, query, 0.0))
            scores = dot_parts(own, key, (((1,), (1,)), ((), ()))) + bias
            top = jnp.max(scores, axis=-1, keepdims=True)
            weights = jnp.exp(scores - top)
            total = jnp.sum(weights, axis=-1, keepdims=True)
            mixed = jnp.where(group == s, dot_parts(halves(weights), value) / total, mixed)
        out_ref[:, n] = mixed.reshape(32, 8, 128)
        return carry

    lax.fori_loop(0, 4, step, 0)


def output_kernel(mixed_ref, gate_ref, rows_ref, weight_ref, out_ref):
    columns = []
    for half in range(2):
        parts = [mixed_ref[:, half * 4 + h].reshape(16, 8, 128) for h in range(4)]
        columns.append(jnp.stack(swap_groups(parts), axis=1).reshape(512, 128))
    gated = jnp.concatenate(columns, axis=1) * gate_ref[...]
    out_ref[...] = rows_ref[...] + dot3(gated, weight_ref[...])


def shape_of(*lengths):
    return jax.ShapeDtypeStruct(lengths, f32)


def call(kernel, name, flops, out_shape, *args, scratch=()):
    return pl.pallas_call(
        kernel,
        out_shape=out_shape,
        scratch_shapes=list(scratch),
        name=name,
        cost_estimate=pl.CostEstimate(flops=flops, bytes_accessed=2**20, transcendentals=0),
        compiler_params=pltpu.CompilerParams(vmem_limit_bytes=40 * 2**20),
    )(*args)


def exchanged(value, axes):
    return lax.all_to_all(value, axes, 0, 0, tiled=True)


def sent_to_all(value, axes):
    count = lax.axis_size(axes)
    return exchanged(jnp.broadcast_to(value[None], (count, *value.shape)), axes)


def on_device(
    alignment,
    pair_features,
    outer_gain,
    w_outer_in,
    w_outer_out,
    pair_gain,
    w_bias,
    row_gain,
    w_project,
    w_output,
):
    rows = alignment.reshape(512, 256)
    w_in = jnp.pad(w_outer_in, ((0, 0), (0, 64)))
    w_out = w_outer_out.reshape(32, 32, 128).transpose(1, 0, 2).reshape(1024, 128)
    y, x, core = (lax.axis_index(axis) for axis in ("yl", "xl", "core"))
    left, right = call(
        maps_kernel,
        "maps",
        10**9,
        (shape_of(2, 64, 128), shape_of(64, 256)),
        rows,
        outer_gain.reshape(256, 1),
        w_in,
        scratch=[pltpu.VMEM((512, 128), f32)],
    )
    moved_rows = exchanged(alignment.reshape(4, 16, 8, 256), "zh").reshape(512, 256)
    left_a = lax.dynamic_index_in_dim(left, y, 0, keepdims=False)
    left_b = lax.dynamic_index_in_dim(left, 1 - y, 0, keepdims=False)
    left_a = lax.ppermute(left_a, ("yl", "xl"), [(0, 0), (1, 2), (2, 1), (3, 3)])
    left_b = lax.ppermute(left_b, ("yl", "xl"), [(0, 1), (1, 3), (2, 0), (3, 2)])
    left_a, left_b, right, moved_rows = lax.optimization_barrier(
        (left_a, left_b, right, moved_rows)
    )
    left = jnp.where(x == y, jnp.stack([left_a, left_b]), jnp.stack([left_b, left_a]))
    left_all = sent_to_all(left, ("zh", "zl")).reshape(8, 2, 64, 128)
    swap = [(0, 1), (1, 0)]
    other = lax.ppermute(right, "core", swap)
    right = jnp.where(core == 0, jnp.stack([right, other]), jnp.stack([other, right]))
    other = lax.ppermute(right, "xl", swap)
    right = jnp.where(x == 0, jnp.concatenate([right, other]), jnp.concatenate([other, right]))
    other = lax.ppermute(right, "yl", swap)
    qkv = call(
        project_kernel,
        "project",
        4 * 10**9,
        shape_of(8, 3, 4, 4, 8, 128),
        moved_rows,
        row_gain.reshape(256, 1),
        w_project,
    )
    qkv, left_all, right, other = lax.optimization_barrier((qkv, left_all, right, other))
    qkv = exchanged(qkv, CUBE)
    gate = call(
        gate_kernel,
        "gate",
        10**9,
        shape_of(512, 256),
        rows,
        row_gain.reshape(256, 1),
        w_project,
    )
    parts = call(
        outer_kernel,
        "outer",
        4 * 10**9,
        shape_of(2, 4, 4, 4, 8, 128),
        left_all,
        right,
        other,
        w_out,
        scratch=[pltpu.VMEM((4, 256, 128), f32), pltpu.VMEM((1024, 128), f32)],
    )
    parts, qkv, gate = lax.optimization_barrier((parts, qkv, gate))
    parts = exchanged(parts.reshape(8, 4, 4, 8, 128), ("xh", "xl", "core"))
    parts = call(
        add_kernel,
        "add",
        10**6,
        shape_of(4, 4, 4, 8, 128),
        parts.reshape(2, 4, 4, 4, 8, 128),
    )
    parts = exchanged(parts, "yh")
    updated_pair, bias = call(
        pair_kernel,
        "pair",
        10**8,
        (shape_of(16, 8, 128), shape_of(8, 128)),
        parts.reshape(4, 16, 8, 128),
        pair_features,
        pair_gain.reshape(1, 128),
        w_bias.T,
    )
    bias = exchanged(jnp.broadcast_to(bias[None], (4, 8, 128)).reshape(32, 128), RES)
    bias = bias.reshape(32, 16, 8).transpose(1, 0, 2).reshape(16, 256)
    bias = sent_to_all(bias, SEQ).reshape(16, 16, 256)
    mixed = call(attend_kernel, "attend", 4 * 10**9, shape_of(32, 4, 8, 128), qkv, bias)
    mixed = exchanged(mixed, RES)
    out = call(
        output_kernel,
        "output",
        10**9,
        shape_of(512, 256),
        mixed.reshape(4, 8, 4, 8, 128),
        gate,
        rows,
        w_output,
    )
    return out.reshape(alignment.shape), updated_pair


def solution(mesh):
    fine = Mesh(
        mesh.devices.reshape(2, 4, 2, 4, 2, 2, 2), ("xh", "yh", "yl", "zh", "zl", "xl", "core")
    )
    tiled = P(SEQ, RES, None)
    return jax.shard_map(
        on_device,
        mesh=fine,
        in_specs=(tiled, tiled) + (P(),) * 8,
        out_specs=(tiled, tiled),
        check_vma=False,
    )
```

```python
import functools

import jax
import jax.numpy as jnp
from jax import lax
from jax.experimental import pallas as pl
from jax.experimental.pallas import tpu as pltpu
from jax.sharding import Mesh, PartitionSpec as P


f32 = jnp.float32
bf16 = jnp.bfloat16
precise = lax.Precision.HIGHEST

SEQ = ("xh", "yh", "yl")
RES = ("zh", "zl", "xl", "core")


def dot6(a, b, dims=(((1,), (0,)), ((), ()))):
    return lax.dot_general(a, b, dims, precision=precise, preferred_element_type=f32)


def halves(x):
    high = x.astype(bf16)
    low = (x - high.astype(f32)).astype(bf16)
    return high, low


def dot_parts(a, b, dims=(((1,), (0,)), ((), ()))):
    dot = functools.partial(lax.dot_general, dimension_numbers=dims, preferred_element_type=f32)
    return dot(a[0], b[0]) + (dot(a[0], b[1]) + dot(a[1], b[0]))


def dot3(a, b, dims=(((1,), (0,)), ((), ()))):
    return dot_parts(halves(a), halves(b), dims)


def center_scale(x):
    average = jnp.mean(x, axis=-1, keepdims=True)
    centered = x - average
    variance = jnp.mean(centered * centered, axis=-1, keepdims=True)
    return centered * lax.rsqrt(variance + 1e-05)


def lane_group(shape):
    return lax.broadcasted_iota(jnp.int32, shape, len(shape) - 1) // 32


def lanes_moved(x, shift):
    rows = x.reshape(-1, 128)
    return pltpu.roll(rows, shift % 128, 1).reshape(x.shape)


def swap_groups(parts):
    group = lane_group(parts[0].shape)
    low = group % 2 == 0
    x = [None] * 4
    for a in (0, 2):
        x[a] = jnp.where(low, parts[a], lanes_moved(parts[a + 1], 32))
        x[a + 1] = jnp.where(low, lanes_moved(parts[a], -32), parts[a + 1])
    first = group < 2
    y = [None] * 4
    for a in (0, 1):
        y[a] = jnp.where(first, x[a], lanes_moved(x[a + 2], 64))
        y[a + 2] = jnp.where(first, lanes_moved(x[a], 64), x[a + 2])
    return y


def maps_kernel(rows_ref, gain_ref, weight_ref, left_ref, right_ref, maps_ref):
    normed = center_scale(rows_ref[...]) * gain_ref[...]
    maps_ref[:, :64] = dot6(normed, weight_ref[...], (((1,), (1,)), ((), ())))
    count = left_ref.shape[1]
    group = lane_group((count, 128))
    for half in range(2):
        left = jnp.zeros((count, 128), f32)
        right = jnp.zeros((count, 128), f32)
        for k in range(4):
            part = maps_ref[pl.ds(half * 4 + k, count, stride=8), :]
            left = jnp.where(group == k, lanes_moved(part, 32 * k), left)
            right = jnp.where(group == k, lanes_moved(part, 32 * k - 32), right)
        left_ref[half] = left
        right_ref[:, half * 128 : half * 128 + 128] = right


def project_kernel(own_ref, rows_ref, gain_ref, weight_ref, qkv_ref):
    normed = halves(center_scale(rows_ref[...]) * gain_ref[...])
    for t in range(3):
        block = dot_parts(normed, halves(weight_ref[:, t * 256 : t * 256 + 256]))
        if t == 0:
            block = block * 32 ** (-0.5)
        for half in range(2):
            part = block[:, half * 128 : half * 128 + 128].reshape(16, 4, 8, 128)
            moved = swap_groups([part[:, s] for s in range(4)])
            for h in range(4):
                own = moved[h].reshape(4, 4, 8, 128)
                z, x, core = half ^ own_ref[0], (h // 2) ^ own_ref[1], (h % 2) ^ own_ref[2]
                for n in range(4):
                    qkv_ref[core, x, z, t, n] = own[:, n]


def gate_kernel(rows_ref, gain_ref, weight_ref, gate_ref):
    normed = center_scale(rows_ref[...]) * gain_ref[...]
    gate_ref[...] = jax.nn.sigmoid(dot3(normed, weight_ref[...]))


def outer_kernel(
    order_ref, left_ref, own_ref, other_ref, weight_ref, out_ref, turned_ref, rows_ref, parts_ref, both_ref
):
    for r in range(4):
        both = jnp.concatenate([own_ref[r], other_ref[r]], axis=0)
        turned_ref[r] = both.T
    for y in range(32):
        for r in range(4):
            rows_ref[(y * 4 + r) * 8 : (y * 4 + r) * 8 + 8, :] = turned_ref[r, pl.ds(y, 8, stride=32), :]
    high, low = halves(rows_ref[...])
    parts_ref[:, :128] = high
    parts_ref[:, 128:] = low
    for y in range(32):
        high, low = halves(weight_ref[pl.ds(y, 32, stride=32), :])
        both_ref[y * 32 : y * 32 + 32, :128] = high
        both_ref[y * 32 : y * 32 + 32, 128:] = low
    dot = functools.partial(jnp.dot, preferred_element_type=f32)

    def step(z, carry):
        left = jnp.concatenate(
            [
                jnp.concatenate([left_ref[2 * z + k, 0], left_ref[2 * z + k, 1]], axis=0)
                for k in range(2)
            ],
            axis=1,
        )
        high, low = halves(left)
        outer = dot(parts_ref[...], jnp.concatenate([high, high], axis=0))
        outer = outer + dot(parts_ref[:, :128], low)
        blocks = []
        for k in range(2):
            own = outer[:, k * 128 : k * 128 + 128].reshape(8, 4, 32, 128)
            moved = swap_groups([own[:, y] for y in range(4)])
            blocks += [jnp.concatenate([moved[i][y] for y in range(8)], axis=1) for i in range(4)]
        high, low = halves(jnp.concatenate(blocks, axis=0))
        update = dot(high, both_ref[...])
        update = update[:, :128] + (update[:, 128:] + dot(low, both_ref[:, :128]))
        update = update.reshape(2, 4, 4, 8, 128)
        for k in range(2):
            for r in range(4):
                out_ref[2 * z + k, r] = update[k, :, r]
        return carry

    lax.fori_loop(0, 4, step, 0)


def pair_kernel(parts_ref, pair_ref, gain_ref, weight_ref, pair_out_ref, bias_ref):
    total = parts_ref[0]
    for g in range(1, 8):
        total = total + parts_ref[g]
    total = total * (1.0 / 1024.0)
    for x in range(2):
        for c in range(2):
            at = c * 8 + x * 4
            pair_out_ref[at : at + 4] = pair_ref[at : at + 4] + total[(x * 2 + c) * 4 : (x * 2 + c) * 4 + 4]
    normed = center_scale(pair_out_ref[...].reshape(128, 128)) * gain_ref[...]
    bias_ref[...] = dot6(weight_ref[...], normed, (((1,), (1,)), ((), ())))


def attend_kernel(own_ref, *refs):
    pieces, (bias_ref, out_ref, qkv_ref) = refs[:8], refs[8:]
    for k in range(8):
        z, x, core = (k // 4) ^ own_ref[0], (k // 2 % 2) ^ own_ref[1], (k % 2) ^ own_ref[2]
        qkv_ref[z * 4 + x * 2 + core] = pieces[k][...]
    bias = bias_ref[...].reshape(256, 256)
    group = lane_group((256, 128))
    dot = functools.partial(jnp.dot, preferred_element_type=f32)
    across = (((1,), (1,)), ((), ()))
    dot_across = functools.partial(
        lax.dot_general, dimension_numbers=across, preferred_element_type=f32
    )

    def residues(t, n):
        return jnp.concatenate([qkv_ref[:, t, n, z].reshape(64, 128) for z in range(4)], axis=0)

    def step(n, carry):
        query = residues(0, n)
        key_high, key_low = halves(residues(1, n))
        keys = jnp.concatenate([key_high, key_high], axis=1)
        value_high, value_low = halves(residues(2, n))
        values = jnp.concatenate([value_high, value_low], axis=1)
        mixed = jnp.zeros((256, 128), f32)
        for s in range(4):
            high, low = halves(jnp.where(group == s, query, 0.0))
            scores = dot_across(jnp.concatenate([high, low], axis=1), keys)
            scores = scores + dot_across(high, key_low) + bias
            top = jnp.max(scores, axis=-1, keepdims=True)
            weights = jnp.exp(scores - top)
            total = jnp.sum(weights, axis=-1, keepdims=True)
            high, low = halves(weights)
            both = dot(high, values)
            summed = both[:, :128] + (both[:, 128:] + dot(low, value_high))
            mixed = jnp.where(group == s, summed / total, mixed)
        out_ref[:, n] = mixed.reshape(32, 8, 128)
        return carry

    lax.fori_loop(0, 4, step, 0)


def output_kernel(mixed_ref, gate_ref, rows_ref, weight_ref, out_ref):
    columns = []
    for half in range(2):
        parts = [mixed_ref[:, half * 4 + h].reshape(16, 8, 128) for h in range(4)]
        columns.append(jnp.stack(swap_groups(parts), axis=1).reshape(512, 128))
    gated = jnp.concatenate(columns, axis=1) * gate_ref[...]
    out_ref[...] = rows_ref[...] + dot3(gated, weight_ref[...])


def shape_of(*lengths):
    return jax.ShapeDtypeStruct(lengths, f32)


def call(kernel, flops, out_shape, *args, scratch=(), scalars=0):
    specs = [pl.BlockSpec(memory_space=pltpu.SMEM)] * scalars
    specs += [pl.BlockSpec(memory_space=pltpu.VMEM)] * (len(args) - scalars)
    return pl.pallas_call(
        kernel,
        in_specs=specs,
        out_shape=out_shape,
        scratch_shapes=list(scratch),
        cost_estimate=pl.CostEstimate(flops=flops, bytes_accessed=2**20, transcendentals=0),
        compiler_params=pltpu.CompilerParams(vmem_limit_bytes=24 * 2**20),
    )(*args)


def exchanged(value, axes):
    return lax.all_to_all(value, axes, 0, 0, tiled=True)


def sent_to_all(value, axes):
    count = lax.axis_size(axes)
    return exchanged(jnp.broadcast_to(value[None], (count, *value.shape)), axes)


def on_device(
    alignment,
    pair_features,
    outer_gain,
    w_outer_in,
    w_outer_out,
    pair_gain,
    w_bias,
    row_gain,
    w_project,
    w_output,
):
    rows = alignment.reshape(512, 256)
    gain = row_gain.reshape(1, 256)
    y, z, x, core = (lax.axis_index(axis) for axis in ("yl", "zl", "xl", "core"))
    own = jnp.stack([z, x, core])
    left, right = call(
        maps_kernel,
        10**9,
        (shape_of(2, 64, 128), shape_of(64, 256)),
        rows,
        outer_gain.reshape(1, 256),
        w_outer_in.T,
        scratch=[pltpu.VMEM((512, 128), f32)],
    )
    gate = call(gate_kernel, 10**9, shape_of(512, 256), rows, gain, w_project[:, 768:])
    moved_rows = exchanged(alignment.reshape(4, 16, 8, 256), "zh").reshape(512, 256)
    left_a = lax.dynamic_index_in_dim(left, y, 0, keepdims=False)
    left_b = lax.dynamic_index_in_dim(left, 1 - y, 0, keepdims=False)
    left_a = lax.ppermute(left_a, ("yl", "xl"), [(0, 0), (1, 2), (2, 1), (3, 3)])
    left_b = lax.ppermute(left_b, ("yl", "xl"), [(0, 1), (1, 3), (2, 0), (3, 2)])
    swap = [(0, 1), (1, 0)]
    other = lax.ppermute(right, "core", swap)
    right = jnp.where(core == 0, jnp.stack([right, other]), jnp.stack([other, right]))
    left_a, left_b, moved_rows, gate = lax.optimization_barrier(
        (left_a, left_b, moved_rows, gate)
    )
    left = jnp.where(x == y, jnp.stack([left_a, left_b]), jnp.stack([left_b, left_a]))
    left_all = sent_to_all(left, ("zh", "zl")).reshape(8, 2, 64, 128)
    other = lax.ppermute(right, "xl", swap)
    right = jnp.where(x == 0, jnp.concatenate([right, other]), jnp.concatenate([other, right]))
    other = lax.ppermute(right, "yl", swap)
    qkv = call(
        project_kernel,
        4 * 10**9,
        shape_of(2, 2, 2, 3, 4, 4, 8, 128),
        own,
        moved_rows,
        gain,
        w_project[:, :768],
        scalars=1,
    )
    order, qkv = lax.optimization_barrier((own, qkv))
    far_core = lax.ppermute(qkv[1], "core", swap)
    far_x = lax.ppermute(qkv[0, 1], "xl", swap)
    parts = call(
        outer_kernel,
        4 * 10**9,
        shape_of(8, 4, 4, 8, 128),
        order,
        left_all,
        right,
        other,
        w_outer_out,
        scratch=[
            pltpu.VMEM((4, 256, 128), f32),
            pltpu.VMEM((1024, 128), f32),
            pltpu.VMEM((1024, 256), bf16),
            pltpu.VMEM((1024, 256), bf16),
        ],
        scalars=1,
    )
    parts, far_core, far_x = lax.optimization_barrier((parts, far_core, far_x))
    parts = exchanged(parts.reshape(32, 4, 8, 128), ("xh", "yh", "xl", "core"))
    pieces = [qkv[0, 0], far_core[0], far_x, lax.ppermute(far_core[1], "xl", swap)]
    moved = [lax.ppermute(p[1], "zl", swap) for p in pieces[:2]]
    kept = [p[0] for p in pieces]
    sent = [p[1] for p in pieces[2:]]
    parts, kept, sent = lax.optimization_barrier((parts, kept, sent))
    updated_pair, bias = call(
        pair_kernel,
        10**8,
        (shape_of(16, 8, 128), shape_of(8, 128)),
        parts.reshape(8, 16, 8, 128),
        pair_features,
        pair_gain.reshape(1, 128),
        w_bias.T,
    )
    bias, sent = lax.optimization_barrier((bias, sent))
    moved += [lax.ppermute(p, "zl", swap) for p in sent]
    pieces = kept + moved
    bias = exchanged(jnp.broadcast_to(bias[None], (4, 8, 128)).reshape(32, 128), RES)
    bias = bias.reshape(32, 16, 8).transpose(1, 0, 2).reshape(16, 256)
    bias = sent_to_all(bias, SEQ).reshape(16, 16, 256)
    mixed = call(
        attend_kernel,
        4 * 10**9,
        shape_of(32, 4, 8, 128),
        own,
        *pieces,
        bias,
        scratch=[pltpu.VMEM((8, 3, 4, 4, 8, 128), f32)],
        scalars=1,
    )
    mixed = exchanged(mixed, RES)
    out = call(
        output_kernel,
        10**9,
        shape_of(512, 256),
        mixed.reshape(4, 8, 4, 8, 128),
        gate,
        rows,
        w_output,
    )
    return out.reshape(alignment.shape), updated_pair


def solution(mesh):
    fine = Mesh(
        mesh.devices.reshape(2, 4, 2, 4, 2, 2, 2), ("xh", "yh", "yl", "zh", "zl", "xl", "core")
    )
    tiled = P(SEQ, RES, None)
    return jax.shard_map(
        on_device,
        mesh=fine,
        in_specs=(tiled, tiled) + (P(),) * 8,
        out_specs=(tiled, tiled),
        check_vma=False,
    )
```

```python
import functools

import jax
import jax.numpy as jnp
from jax import lax
from jax.experimental import pallas as pl
from jax.experimental.pallas import tpu as pltpu
from jax.sharding import Mesh, PartitionSpec as P


f32 = jnp.float32
bf16 = jnp.bfloat16
precise = lax.Precision.HIGHEST

SEQ = ("xh", "yh", "yl")
RES = ("zh", "zl", "xl", "core")


def dot6(a, b, dims=(((1,), (0,)), ((), ()))):
    return lax.dot_general(a, b, dims, precision=precise, preferred_element_type=f32)


def halves(x):
    high = x.astype(bf16)
    low = (x - high.astype(f32)).astype(bf16)
    return high, low


def dot_parts(a, b, dims=(((1,), (0,)), ((), ()))):
    dot = functools.partial(lax.dot_general, dimension_numbers=dims, preferred_element_type=f32)
    return dot(a[0], b[0]) + (dot(a[0], b[1]) + dot(a[1], b[0]))


def dot3(a, b, dims=(((1,), (0,)), ((), ()))):
    return dot_parts(halves(a), halves(b), dims)


def center_scale(x):
    average = jnp.mean(x, axis=-1, keepdims=True)
    centered = x - average
    variance = jnp.mean(centered * centered, axis=-1, keepdims=True)
    return centered * lax.rsqrt(variance + 1e-05)


def lane_group(shape):
    return lax.broadcasted_iota(jnp.int32, shape, len(shape) - 1) // 32


def lanes_moved(x, shift):
    rows = x.reshape(-1, 128)
    return pltpu.roll(rows, shift % 128, 1).reshape(x.shape)


def swap_groups(parts):
    group = lane_group(parts[0].shape)
    low = group % 2 == 0
    x = [None] * 4
    for a in (0, 2):
        x[a] = jnp.where(low, parts[a], lanes_moved(parts[a + 1], 32))
        x[a + 1] = jnp.where(low, lanes_moved(parts[a], -32), parts[a + 1])
    first = group < 2
    y = [None] * 4
    for a in (0, 1):
        y[a] = jnp.where(first, x[a], lanes_moved(x[a + 2], 64))
        y[a + 2] = jnp.where(first, lanes_moved(x[a], 64), x[a + 2])
    return y


def maps_kernel(rows_ref, gain_ref, weight_ref, left_ref, right_ref, maps_ref):
    normed = center_scale(rows_ref[...]) * gain_ref[...]
    maps_ref[:, :64] = dot6(normed, weight_ref[...], (((1,), (1,)), ((), ())))
    count = left_ref.shape[1]
    group = lane_group((count, 128))
    for half in range(2):
        left = jnp.zeros((count, 128), f32)
        right = jnp.zeros((count, 128), f32)
        for k in range(4):
            part = maps_ref[pl.ds(half * 4 + k, count, stride=8), :]
            left = jnp.where(group == k, lanes_moved(part, 32 * k), left)
            right = jnp.where(group == k, lanes_moved(part, 32 * k - 32), right)
        left_ref[half] = left
        right_ref[:, half * 128 : half * 128 + 128] = right


def project_kernel(own_ref, rows_ref, gain_ref, weight_ref, qkv_ref):
    normed = halves(center_scale(rows_ref[...]) * gain_ref[...])
    for t in range(3):
        block = dot_parts(normed, halves(weight_ref[:, t * 256 : t * 256 + 256]))
        if t == 0:
            block = block * 32 ** (-0.5)
        for half in range(2):
            part = block[:, half * 128 : half * 128 + 128].reshape(16, 4, 8, 128)
            moved = swap_groups([part[:, s] for s in range(4)])
            for h in range(4):
                own = moved[h].reshape(4, 4, 8, 128)
                z, x, core = half ^ own_ref[0], (h // 2) ^ own_ref[1], (h % 2) ^ own_ref[2]
                for n in range(4):
                    qkv_ref[core, x, z, t, n] = own[:, n]


def gate_kernel(rows_ref, gain_ref, weight_ref, gate_ref):
    normed = center_scale(rows_ref[...]) * gain_ref[...]
    gate_ref[...] = jax.nn.sigmoid(dot3(normed, weight_ref[...]))


def outer_kernel(
    order_ref, left_ref, own_ref, other_ref, weight_ref, out_ref, turned_ref, rows_ref, parts_ref, both_ref
):
    for r in range(4):
        both = jnp.concatenate([own_ref[r], other_ref[r]], axis=0)
        turned_ref[r] = both.T
    for y in range(32):
        for r in range(4):
            rows_ref[(y * 4 + r) * 8 : (y * 4 + r) * 8 + 8, :] = turned_ref[r, pl.ds(y, 8, stride=32), :]
    high, low = halves(rows_ref[...])
    parts_ref[:, :128] = high
    parts_ref[:, 128:] = low
    for y in range(32):
        high, low = halves(weight_ref[pl.ds(y, 32, stride=32), :])
        both_ref[y * 32 : y * 32 + 32, :128] = high
        both_ref[y * 32 : y * 32 + 32, 128:] = low
    dot = functools.partial(jnp.dot, preferred_element_type=f32)

    for z in range(4):
        left = jnp.concatenate(
            [
                jnp.concatenate([left_ref[2 * z + k, 0], left_ref[2 * z + k, 1]], axis=0)
                for k in range(2)
            ],
            axis=1,
        )
        high, low = halves(left)
        outer = dot(parts_ref[...], jnp.concatenate([high, high], axis=0))
        outer = outer + dot(parts_ref[:, :128], low)
        blocks = []
        for k in range(2):
            own = outer[:, k * 128 : k * 128 + 128].reshape(8, 4, 32, 128)
            moved = swap_groups([own[:, y] for y in range(4)])
            blocks += [jnp.concatenate([moved[i][y] for y in range(8)], axis=1) for i in range(4)]
        high, low = halves(jnp.concatenate(blocks, axis=0))
        update = dot(high, both_ref[...])
        update = update[:, :128] + (update[:, 128:] + dot(low, both_ref[:, :128]))
        update = update.reshape(2, 4, 4, 8, 128)
        for k in range(2):
            for r in range(4):
                out_ref[2 * z + k, r] = update[k, :, r]


def pair_kernel(parts_ref, pair_ref, gain_ref, weight_ref, pair_out_ref, bias_ref):
    total = parts_ref[0]
    for g in range(1, 8):
        total = total + parts_ref[g]
    total = total * (1.0 / 1024.0)
    for x in range(2):
        for c in range(2):
            at = c * 8 + x * 4
            pair_out_ref[at : at + 4] = pair_ref[at : at + 4] + total[(x * 2 + c) * 4 : (x * 2 + c) * 4 + 4]
    normed = center_scale(pair_out_ref[...].reshape(128, 128)) * gain_ref[...]
    bias = dot6(weight_ref[...], normed, (((1,), (1,)), ((), ())))
    for copy in range(4):
        bias_ref[copy] = bias


def attend_kernel(own_ref, *refs):
    pieces, (bias_ref, out_ref, qkv_ref) = refs[:8], refs[8:]
    for k in range(8):
        z, x, core = (k // 4) ^ own_ref[0], (k // 2 % 2) ^ own_ref[1], (k % 2) ^ own_ref[2]
        qkv_ref[z * 4 + x * 2 + core] = pieces[k][...]
    bias = bias_ref[...].reshape(256, 256)
    group = lane_group((256, 128))
    dot = functools.partial(jnp.dot, preferred_element_type=f32)
    across = (((1,), (1,)), ((), ()))
    dot_across = functools.partial(
        lax.dot_general, dimension_numbers=across, preferred_element_type=f32
    )

    def residues(t, n):
        return jnp.concatenate([qkv_ref[:, t, n, z].reshape(64, 128) for z in range(4)], axis=0)

    def step(n, carry):
        query = residues(0, n)
        key_high, key_low = halves(residues(1, n))
        keys = jnp.concatenate([key_high, key_high], axis=1)
        value_high, value_low = halves(residues(2, n))
        values = jnp.concatenate([value_high, value_low], axis=1)
        mixed = jnp.zeros((256, 128), f32)
        for s in range(4):
            high, low = halves(jnp.where(group == s, query, 0.0))
            scores = dot_across(jnp.concatenate([high, low], axis=1), keys)
            scores = scores + dot_across(high, key_low) + bias
            top = jnp.max(scores, axis=-1, keepdims=True)
            weights = jnp.exp(scores - top)
            total = jnp.sum(weights, axis=-1, keepdims=True)
            high, low = halves(weights)
            both = dot(high, values)
            summed = both[:, :128] + (both[:, 128:] + dot(low, value_high))
            mixed = jnp.where(group == s, summed / total, mixed)
        out_ref[:, n] = mixed.reshape(32, 8, 128)
        return carry

    lax.fori_loop(0, 4, step, 0)


def output_kernel(mixed_ref, gate_ref, rows_ref, weight_ref, out_ref):
    columns = []
    for half in range(2):
        parts = [mixed_ref[:, half * 4 + h].reshape(16, 8, 128) for h in range(4)]
        columns.append(jnp.stack(swap_groups(parts), axis=1).reshape(512, 128))
    gated = jnp.concatenate(columns, axis=1) * gate_ref[...]
    out_ref[...] = rows_ref[...] + dot3(gated, weight_ref[...])


def shape_of(*lengths):
    return jax.ShapeDtypeStruct(lengths, f32)


def call(kernel, flops, out_shape, *args, scratch=(), scalars=0):
    specs = [pl.BlockSpec(memory_space=pltpu.SMEM)] * scalars
    specs += [pl.BlockSpec(memory_space=pltpu.VMEM)] * (len(args) - scalars)
    return pl.pallas_call(
        kernel,
        in_specs=specs,
        out_shape=out_shape,
        scratch_shapes=list(scratch),
        cost_estimate=pl.CostEstimate(flops=flops, bytes_accessed=2**20, transcendentals=0),
        compiler_params=pltpu.CompilerParams(vmem_limit_bytes=24 * 2**20),
    )(*args)


def exchanged(value, axes):
    return lax.all_to_all(value, axes, 0, 0, tiled=True)


def sent_to_all(value, axes):
    count = lax.axis_size(axes)
    return exchanged(jnp.broadcast_to(value[None], (count, *value.shape)), axes)


def on_device(
    alignment,
    pair_features,
    outer_gain,
    w_outer_in,
    w_outer_out,
    pair_gain,
    w_bias,
    row_gain,
    w_project,
    w_output,
):
    rows = alignment.reshape(512, 256)
    gain = row_gain.reshape(1, 256)
    y, z, x, core = (lax.axis_index(axis) for axis in ("yl", "zl", "xl", "core"))
    own = jnp.stack([z, x, core])
    left, right = call(
        maps_kernel,
        10**9,
        (shape_of(2, 64, 128), shape_of(64, 256)),
        rows,
        outer_gain.reshape(1, 256),
        w_outer_in.T,
        scratch=[pltpu.VMEM((512, 128), f32)],
    )
    moved_rows = exchanged(alignment.reshape(4, 16, 8, 256), "zh").reshape(512, 256)
    left_a = lax.dynamic_index_in_dim(left, y, 0, keepdims=False)
    left_b = lax.dynamic_index_in_dim(left, 1 - y, 0, keepdims=False)
    left_a = lax.ppermute(left_a, ("yl", "xl"), [(0, 0), (1, 2), (2, 1), (3, 3)])
    left_b = lax.ppermute(left_b, ("yl", "xl"), [(0, 1), (1, 3), (2, 0), (3, 2)])
    swap = [(0, 1), (1, 0)]
    other = lax.ppermute(right, "core", swap)
    right = jnp.where(core == 0, jnp.stack([right, other]), jnp.stack([other, right]))
    left_a, left_b, moved_rows = lax.optimization_barrier((left_a, left_b, moved_rows))
    left = jnp.where(x == y, jnp.stack([left_a, left_b]), jnp.stack([left_b, left_a]))
    left_all = sent_to_all(left, ("zh", "zl")).reshape(8, 2, 64, 128)
    other = lax.ppermute(right, "xl", swap)
    right = jnp.where(x == 0, jnp.concatenate([right, other]), jnp.concatenate([other, right]))
    other = lax.ppermute(right, "yl", swap)
    qkv = call(
        project_kernel,
        4 * 10**9,
        shape_of(2, 2, 2, 3, 4, 4, 8, 128),
        own,
        moved_rows,
        gain,
        w_project[:, :768],
        scalars=1,
    )
    order, qkv = lax.optimization_barrier((own, qkv))
    far_core = lax.ppermute(qkv[1], "core", swap)
    far_x = lax.ppermute(qkv[0, 1], "xl", swap)
    parts = call(
        outer_kernel,
        4 * 10**9,
        shape_of(8, 4, 4, 8, 128),
        order,
        left_all,
        right,
        other,
        w_outer_out,
        scratch=[
            pltpu.VMEM((4, 256, 128), f32),
            pltpu.VMEM((1024, 128), f32),
            pltpu.VMEM((1024, 256), bf16),
            pltpu.VMEM((1024, 256), bf16),
        ],
        scalars=1,
    )
    parts, far_core, far_x = lax.optimization_barrier((parts, far_core, far_x))
    parts = exchanged(parts.reshape(32, 4, 8, 128), ("xh", "yh", "xl", "core"))
    pieces = [qkv[0, 0], far_core[0], far_x, lax.ppermute(far_core[1], "xl", swap)]
    moved = [lax.ppermute(p[1], "zl", swap) for p in pieces[:3]]
    kept = [p[0] for p in pieces]
    sent = pieces[3][1]
    parts, kept, sent = lax.optimization_barrier((parts, kept, sent))
    updated_pair, bias = call(
        pair_kernel,
        10**8,
        (shape_of(16, 8, 128), shape_of(4, 8, 128)),
        parts.reshape(8, 16, 8, 128),
        pair_features,
        pair_gain.reshape(1, 128),
        w_bias.T,
    )
    bias, sent, late_gain = lax.optimization_barrier((bias, sent, gain))
    gate = call(gate_kernel, 10**9, shape_of(512, 256), rows, late_gain, w_project[:, 768:])
    moved.append(lax.ppermute(sent, "zl", swap))
    pieces = kept + moved
    bias = exchanged(bias.reshape(32, 128), RES)
    bias = bias.reshape(32, 16, 8).transpose(1, 0, 2).reshape(16, 256)
    bias, pieces, gate = lax.optimization_barrier((bias, pieces, gate))
    bias = sent_to_all(bias, SEQ).reshape(16, 16, 256)
    mixed = call(
        attend_kernel,
        4 * 10**9,
        shape_of(32, 4, 8, 128),
        own,
        *pieces,
        bias,
        scratch=[pltpu.VMEM((8, 3, 4, 4, 8, 128), f32)],
        scalars=1,
    )
    mixed = exchanged(mixed, RES)
    out = call(
        output_kernel,
        10**9,
        shape_of(512, 256),
        mixed.reshape(4, 8, 4, 8, 128),
        gate,
        rows,
        w_output,
    )
    return out.reshape(alignment.shape), updated_pair


def solution(mesh):
    fine = Mesh(
        mesh.devices.reshape(2, 4, 2, 4, 2, 2, 2), ("xh", "yh", "yl", "zh", "zl", "xl", "core")
    )
    tiled = P(SEQ, RES, None)
    return jax.shard_map(
        on_device,
        mesh=fine,
        in_specs=(tiled, tiled) + (P(),) * 8,
        out_specs=(tiled, tiled),
        check_vma=False,
    )
```

```python
import functools

import jax
import jax.numpy as jnp
from jax import lax
from jax.experimental import pallas as pl
from jax.experimental.pallas import tpu as pltpu
from jax.sharding import Mesh, PartitionSpec as P


f32 = jnp.float32
bf16 = jnp.bfloat16
precise = lax.Precision.HIGHEST

SEQ = ("xh", "yh", "yl")
RES = ("zh", "zl", "xl", "core")


def dot6(a, b, dims=(((1,), (0,)), ((), ()))):
    return lax.dot_general(a, b, dims, precision=precise, preferred_element_type=f32)


def halves(x):
    high = x.astype(bf16)
    low = (x - high.astype(f32)).astype(bf16)
    return high, low


def dot_parts(a, b, dims=(((1,), (0,)), ((), ()))):
    dot = functools.partial(lax.dot_general, dimension_numbers=dims, preferred_element_type=f32)
    return dot(a[0], b[0]) + (dot(a[0], b[1]) + dot(a[1], b[0]))


def dot3(a, b, dims=(((1,), (0,)), ((), ()))):
    return dot_parts(halves(a), halves(b), dims)


def center_scale(x):
    average = jnp.mean(x, axis=-1, keepdims=True)
    centered = x - average
    variance = jnp.mean(centered * centered, axis=-1, keepdims=True)
    return centered * lax.rsqrt(variance + 1e-05)


def lane_group(shape):
    return lax.broadcasted_iota(jnp.int32, shape, len(shape) - 1) // 32


def lanes_moved(x, shift):
    rows = x.reshape(-1, 128)
    return pltpu.roll(rows, shift % 128, 1).reshape(x.shape)


def swap_groups(parts):
    group = lane_group(parts[0].shape)
    low = group % 2 == 0
    x = [None] * 4
    for a in (0, 2):
        x[a] = jnp.where(low, parts[a], lanes_moved(parts[a + 1], 32))
        x[a + 1] = jnp.where(low, lanes_moved(parts[a], -32), parts[a + 1])
    first = group < 2
    y = [None] * 4
    for a in (0, 1):
        y[a] = jnp.where(first, x[a], lanes_moved(x[a + 2], 64))
        y[a + 2] = jnp.where(first, lanes_moved(x[a], 64), x[a + 2])
    return y


def maps_kernel(rows_ref, gain_ref, weight_ref, left_ref, right_ref, maps_ref):
    normed = center_scale(rows_ref[...]) * gain_ref[...]
    maps_ref[:, :64] = dot6(normed, weight_ref[...], (((1,), (1,)), ((), ())))
    count = left_ref.shape[1]
    group = lane_group((count, 128))
    for half in range(2):
        left = jnp.zeros((count, 128), f32)
        right = jnp.zeros((count, 128), f32)
        for k in range(4):
            part = maps_ref[pl.ds(half * 4 + k, count, stride=8), :]
            left = jnp.where(group == k, lanes_moved(part, 32 * k), left)
            right = jnp.where(group == k, lanes_moved(part, 32 * k - 32), right)
        left_ref[half] = left
        right_ref[:, half * 128 : half * 128 + 128] = right


def project_kernel(own_ref, rows_ref, gain_ref, weight_ref, qkv_ref):
    normed = halves(center_scale(rows_ref[...]) * gain_ref[...])
    for t in range(3):
        block = dot_parts(normed, halves(weight_ref[:, t * 256 : t * 256 + 256]))
        if t == 0:
            block = block * 32 ** (-0.5)
        for half in range(2):
            part = block[:, half * 128 : half * 128 + 128].reshape(16, 4, 8, 128)
            moved = swap_groups([part[:, s] for s in range(4)])
            for h in range(4):
                own = moved[h].reshape(4, 4, 8, 128)
                z, x, core = half ^ own_ref[0], (h // 2) ^ own_ref[1], (h % 2) ^ own_ref[2]
                for n in range(4):
                    qkv_ref[core, x, z, t, n] = own[:, n]


def gate_kernel(rows_ref, gain_ref, weight_ref, gate_ref):
    normed = center_scale(rows_ref[...]) * gain_ref[...]
    gate_ref[...] = jax.nn.sigmoid(dot3(normed, weight_ref[...]))


def outer_kernel(
    order_ref, left_ref, own_ref, other_ref, weight_ref, out_ref, turned_ref, rows_ref, parts_ref, both_ref
):
    for r in range(4):
        both = jnp.concatenate([own_ref[r], other_ref[r]], axis=0)
        turned_ref[r] = both.T
    for y in range(32):
        for r in range(4):
            rows_ref[(y * 4 + r) * 8 : (y * 4 + r) * 8 + 8, :] = turned_ref[r, pl.ds(y, 8, stride=32), :]
    high, low = halves(rows_ref[...])
    parts_ref[:, :128] = high
    parts_ref[:, 128:] = low
    for y in range(32):
        high, low = halves(weight_ref[pl.ds(y, 32, stride=32), :])
        both_ref[y * 32 : y * 32 + 32, :128] = high
        both_ref[y * 32 : y * 32 + 32, 128:] = low
    dot = functools.partial(jnp.dot, preferred_element_type=f32)

    for z in range(4):
        left = jnp.concatenate(
            [
                jnp.concatenate([left_ref[2 * z + k, 0], left_ref[2 * z + k, 1]], axis=0)
                for k in range(2)
            ],
            axis=1,
        )
        high, low = halves(left)
        outer = dot(parts_ref[...], jnp.concatenate([high, high], axis=0))
        outer = outer + dot(parts_ref[:, :128], low)
        blocks = []
        for k in range(2):
            own = outer[:, k * 128 : k * 128 + 128].reshape(8, 4, 32, 128)
            moved = swap_groups([own[:, y] for y in range(4)])
            blocks += [jnp.concatenate([moved[i][y] for y in range(8)], axis=1) for i in range(4)]
        high, low = halves(jnp.concatenate(blocks, axis=0))
        update = dot(high, both_ref[...])
        update = update[:, :128] + (update[:, 128:] + dot(low, both_ref[:, :128]))
        update = update.reshape(2, 4, 4, 8, 128)
        for k in range(2):
            for r in range(4):
                out_ref[2 * z + k, r] = update[k, :, r]


def pair_kernel(parts_ref, pair_ref, gain_ref, weight_ref, pair_out_ref, bias_ref):
    total = parts_ref[0]
    for g in range(1, 8):
        total = total + parts_ref[g]
    total = total * (1.0 / 1024.0)
    for x in range(2):
        for c in range(2):
            at = c * 8 + x * 4
            pair_out_ref[at : at + 4] = pair_ref[at : at + 4] + total[(x * 2 + c) * 4 : (x * 2 + c) * 4 + 4]
    normed = center_scale(pair_out_ref[...].reshape(128, 128)) * gain_ref[...]
    bias = dot6(weight_ref[...], normed, (((1,), (1,)), ((), ())))
    for copy in range(4):
        bias_ref[copy] = bias


def attend_kernel(own_ref, *refs):
    kept, moved, (bias_ref, out_ref, qkv_ref) = refs[:4], refs[4:6], refs[6:]
    pieces = list(kept) + [moved[k % 2].at[k // 2] for k in range(4)]
    for k in range(8):
        z, x, core = (k // 4) ^ own_ref[0], (k // 2 % 2) ^ own_ref[1], (k % 2) ^ own_ref[2]
        qkv_ref[z * 4 + x * 2 + core] = pieces[k][...]
    bias = bias_ref[...].reshape(256, 256)
    group = lane_group((256, 128))
    dot = functools.partial(jnp.dot, preferred_element_type=f32)
    across = (((1,), (1,)), ((), ()))
    dot_across = functools.partial(
        lax.dot_general, dimension_numbers=across, preferred_element_type=f32
    )

    def residues(t, n):
        return jnp.concatenate([qkv_ref[:, t, n, z].reshape(64, 128) for z in range(4)], axis=0)

    def step(n, carry):
        query = residues(0, n)
        key_high, key_low = halves(residues(1, n))
        keys = jnp.concatenate([key_high, key_high], axis=1)
        value_high, value_low = halves(residues(2, n))
        values = jnp.concatenate([value_high, value_low], axis=1)
        mixed = jnp.zeros((256, 128), f32)
        for s in range(4):
            high, low = halves(jnp.where(group == s, query, 0.0))
            scores = dot_across(jnp.concatenate([high, low], axis=1), keys)
            scores = scores + dot_across(high, key_low) + bias
            top = jnp.max(scores, axis=-1, keepdims=True)
            weights = jnp.exp(scores - top)
            total = jnp.sum(weights, axis=-1, keepdims=True)
            high, low = halves(weights)
            both = dot(high, values)
            summed = both[:, :128] + (both[:, 128:] + dot(low, value_high))
            mixed = jnp.where(group == s, summed / total, mixed)
        out_ref[:, n] = mixed.reshape(32, 8, 128)
        return carry

    lax.fori_loop(0, 4, step, 0)


def output_kernel(mixed_ref, gate_ref, rows_ref, weight_ref, out_ref):
    columns = []
    for half in range(2):
        parts = [mixed_ref[:, half * 4 + h].reshape(16, 8, 128) for h in range(4)]
        columns.append(jnp.stack(swap_groups(parts), axis=1).reshape(512, 128))
    gated = jnp.concatenate(columns, axis=1) * gate_ref[...]
    out_ref[...] = rows_ref[...] + dot3(gated, weight_ref[...])


def shape_of(*lengths):
    return jax.ShapeDtypeStruct(lengths, f32)


def call(kernel, flops, out_shape, *args, scratch=(), scalars=0):
    specs = [pl.BlockSpec(memory_space=pltpu.SMEM)] * scalars
    specs += [pl.BlockSpec(memory_space=pltpu.VMEM)] * (len(args) - scalars)
    return pl.pallas_call(
        kernel,
        in_specs=specs,
        out_shape=out_shape,
        scratch_shapes=list(scratch),
        cost_estimate=pl.CostEstimate(flops=flops, bytes_accessed=2**20, transcendentals=0),
        compiler_params=pltpu.CompilerParams(vmem_limit_bytes=24 * 2**20),
    )(*args)


def exchanged(value, axes):
    return lax.all_to_all(value, axes, 0, 0, tiled=True)


def sent_to_all(value, axes):
    count = lax.axis_size(axes)
    return exchanged(jnp.broadcast_to(value[None], (count, *value.shape)), axes)


def on_device(
    alignment,
    pair_features,
    outer_gain,
    w_outer_in,
    w_outer_out,
    pair_gain,
    w_bias,
    row_gain,
    w_project,
    w_output,
):
    rows = alignment.reshape(512, 256)
    gain = row_gain.reshape(1, 256)
    y, z, x, core = (lax.axis_index(axis) for axis in ("yl", "zl", "xl", "core"))
    own = jnp.stack([z, x, core])
    left, right = call(
        maps_kernel,
        10**9,
        (shape_of(2, 64, 128), shape_of(64, 256)),
        rows,
        outer_gain.reshape(1, 256),
        w_outer_in.T,
        scratch=[pltpu.VMEM((512, 128), f32)],
    )
    moved_rows = exchanged(alignment.reshape(4, 16, 8, 256), "zh").reshape(512, 256)
    left_a = lax.dynamic_index_in_dim(left, y, 0, keepdims=False)
    left_b = lax.dynamic_index_in_dim(left, 1 - y, 0, keepdims=False)
    left_a = lax.ppermute(left_a, ("yl", "xl"), [(0, 0), (1, 2), (2, 1), (3, 3)])
    left_b = lax.ppermute(left_b, ("yl", "xl"), [(0, 1), (1, 3), (2, 0), (3, 2)])
    swap = [(0, 1), (1, 0)]
    other = lax.ppermute(right, "core", swap)
    right = jnp.where(core == 0, jnp.stack([right, other]), jnp.stack([other, right]))
    left_a, left_b, moved_rows = lax.optimization_barrier((left_a, left_b, moved_rows))
    left = jnp.where(x == y, jnp.stack([left_a, left_b]), jnp.stack([left_b, left_a]))
    left_all = sent_to_all(left, ("zh", "zl")).reshape(8, 2, 64, 128)
    other = lax.ppermute(right, "xl", swap)
    right = jnp.where(x == 0, jnp.concatenate([right, other]), jnp.concatenate([other, right]))
    other = lax.ppermute(right, "yl", swap)
    qkv = call(
        project_kernel,
        4 * 10**9,
        shape_of(2, 2, 2, 3, 4, 4, 8, 128),
        own,
        moved_rows,
        gain,
        w_project[:, :768],
        scalars=1,
    )
    order, qkv = lax.optimization_barrier((own, qkv))
    far_core = lax.ppermute(qkv[1], "core", swap)
    far_x = lax.ppermute(qkv[0, 1], "xl", swap)
    parts = call(
        outer_kernel,
        4 * 10**9,
        shape_of(8, 4, 4, 8, 128),
        order,
        left_all,
        right,
        other,
        w_outer_out,
        scratch=[
            pltpu.VMEM((4, 256, 128), f32),
            pltpu.VMEM((1024, 128), f32),
            pltpu.VMEM((1024, 256), bf16),
            pltpu.VMEM((1024, 256), bf16),
        ],
        scalars=1,
    )
    parts, far_core = lax.optimization_barrier((parts, far_core))
    parts = exchanged(parts.reshape(32, 4, 8, 128), ("xh", "yh", "xl", "core"))
    last = lax.ppermute(far_core[1], "xl", swap)
    moved = lax.ppermute(jnp.stack([qkv[0, 0, 1], far_x[1]]), "zl", swap)
    kept = [qkv[0, 0, 0], far_core[0, 0], far_x[0], last[0]]
    sent = jnp.stack([far_core[0, 1], last[1]])
    parts, kept, sent = lax.optimization_barrier((parts, kept, sent))
    updated_pair, bias = call(
        pair_kernel,
        10**8,
        (shape_of(16, 8, 128), shape_of(4, 8, 128)),
        parts.reshape(8, 16, 8, 128),
        pair_features,
        pair_gain.reshape(1, 128),
        w_bias.T,
    )
    bias, sent = lax.optimization_barrier((bias, sent))
    pieces = kept + [moved, lax.ppermute(sent, "zl", swap)]
    bias = exchanged(bias.reshape(32, 128), RES)
    bias = bias.reshape(32, 16, 8).transpose(1, 0, 2).reshape(16, 256)
    late_gain, bias = lax.optimization_barrier((gain, bias))
    gate = call(gate_kernel, 10**9, shape_of(512, 256), rows, late_gain, w_project[:, 768:])
    bias = sent_to_all(bias, SEQ).reshape(16, 16, 256)
    bias, gate = lax.optimization_barrier((bias, gate))
    mixed = call(
        attend_kernel,
        4 * 10**9,
        shape_of(32, 4, 8, 128),
        own,
        *pieces,
        bias,
        scratch=[pltpu.VMEM((8, 3, 4, 4, 8, 128), f32)],
        scalars=1,
    )
    mixed = exchanged(mixed, RES)
    out = call(
        output_kernel,
        10**9,
        shape_of(512, 256),
        mixed.reshape(4, 8, 4, 8, 128),
        gate,
        rows,
        w_output,
    )
    return out.reshape(alignment.shape), updated_pair


def solution(mesh):
    fine = Mesh(
        mesh.devices.reshape(2, 4, 2, 4, 2, 2, 2), ("xh", "yh", "yl", "zh", "zl", "xl", "core")
    )
    tiled = P(SEQ, RES, None)
    return jax.shard_map(
        on_device,
        mesh=fine,
        in_specs=(tiled, tiled) + (P(),) * 8,
        out_specs=(tiled, tiled),
        check_vma=False,
    )
```

```python
import functools

import jax
import jax.numpy as jnp
from jax import lax
from jax.experimental import pallas as pl
from jax.experimental.pallas import tpu as pltpu
from jax.sharding import Mesh, PartitionSpec as P


f32 = jnp.float32
bf16 = jnp.bfloat16
precise = lax.Precision.HIGHEST

SEQ = ("xh", "yh", "yl")
RES = ("zh", "zl", "xl", "core")


def dot6(a, b, dims=(((1,), (0,)), ((), ()))):
    return lax.dot_general(a, b, dims, precision=precise, preferred_element_type=f32)


def halves(x):
    high = x.astype(bf16)
    low = (x - high.astype(f32)).astype(bf16)
    return high, low


def dot_parts(a, b, dims=(((1,), (0,)), ((), ()))):
    dot = functools.partial(lax.dot_general, dimension_numbers=dims, preferred_element_type=f32)
    return dot(a[0], b[0]) + (dot(a[0], b[1]) + dot(a[1], b[0]))


def dot3(a, b, dims=(((1,), (0,)), ((), ()))):
    return dot_parts(halves(a), halves(b), dims)


def center_scale(x):
    average = jnp.mean(x, axis=-1, keepdims=True)
    centered = x - average
    variance = jnp.mean(centered * centered, axis=-1, keepdims=True)
    return centered * lax.rsqrt(variance + 1e-05)


def lane_group(shape):
    return lax.broadcasted_iota(jnp.int32, shape, len(shape) - 1) // 32


def lanes_moved(x, shift):
    rows = x.reshape(-1, 128)
    return pltpu.roll(rows, shift % 128, 1).reshape(x.shape)


def swap_groups(parts):
    group = lane_group(parts[0].shape)
    low = group % 2 == 0
    x = [None] * 4
    for a in (0, 2):
        x[a] = jnp.where(low, parts[a], lanes_moved(parts[a + 1], 32))
        x[a + 1] = jnp.where(low, lanes_moved(parts[a], -32), parts[a + 1])
    first = group < 2
    y = [None] * 4
    for a in (0, 1):
        y[a] = jnp.where(first, x[a], lanes_moved(x[a + 2], 64))
        y[a + 2] = jnp.where(first, lanes_moved(x[a], 64), x[a + 2])
    return y


def maps_kernel(rows_ref, weight_ref, left_ref, right_ref, maps_ref):
    normed = center_scale(rows_ref[...])
    maps_ref[:, :64] = dot6(normed, weight_ref[...], (((1,), (1,)), ((), ())))
    count = left_ref.shape[1]
    group = lane_group((count, 128))
    for half in range(2):
        left = jnp.zeros((count, 128), f32)
        right = jnp.zeros((count, 128), f32)
        for k in range(4):
            part = maps_ref[pl.ds(half * 4 + k, count, stride=8), :]
            left = jnp.where(group == k, lanes_moved(part, 32 * k), left)
            right = jnp.where(group == k, lanes_moved(part, 32 * k - 32), right)
        left_ref[half] = left
        right_ref[:, half * 128 : half * 128 + 128] = right


def project_kernel(own_ref, rows_ref, gain_ref, weight_ref, qkv_ref):
    normed = halves(center_scale(rows_ref[...]) * gain_ref[...])
    for t in range(3):
        block = dot_parts(normed, halves(weight_ref[:, t * 256 : t * 256 + 256]))
        if t == 0:
            block = block * 32 ** (-0.5)
        for half in range(2):
            part = block[:, half * 128 : half * 128 + 128].reshape(16, 4, 8, 128)
            moved = swap_groups([part[:, s] for s in range(4)])
            for h in range(4):
                own = moved[h].reshape(4, 4, 8, 128)
                z, x, core = half ^ own_ref[0], (h // 2) ^ own_ref[1], (h % 2) ^ own_ref[2]
                for n in range(4):
                    qkv_ref[core, x, z, t, n] = own[:, n]


def gate_kernel(rows_ref, gain_ref, weight_ref, gate_ref):
    normed = center_scale(rows_ref[...]) * gain_ref[...]
    gate_ref[...] = jax.nn.sigmoid(dot3(normed, weight_ref[...]))


def outer_kernel(
    order_ref, left_ref, own_ref, other_ref, weight_ref, out_ref, turned_ref, rows_ref, parts_ref, both_ref
):
    for r in range(4):
        both = jnp.concatenate([own_ref[r], other_ref[r]], axis=0)
        turned_ref[r] = both.T
    for y in range(32):
        for r in range(4):
            rows_ref[(y * 4 + r) * 8 : (y * 4 + r) * 8 + 8, :] = turned_ref[r, pl.ds(y, 8, stride=32), :]
    high, low = halves(rows_ref[...])
    parts_ref[:, :128] = high
    parts_ref[:, 128:] = low
    for y in range(32):
        high, low = halves(weight_ref[pl.ds(y, 32, stride=32), :])
        both_ref[y * 32 : y * 32 + 32, :128] = high
        both_ref[y * 32 : y * 32 + 32, 128:] = low
    dot = functools.partial(jnp.dot, preferred_element_type=f32)

    for z in range(4):
        left = jnp.concatenate(
            [
                jnp.concatenate([left_ref[2 * z + k, 0], left_ref[2 * z + k, 1]], axis=0)
                for k in range(2)
            ],
            axis=1,
        )
        high, low = halves(left)
        outer = dot(parts_ref[...], jnp.concatenate([high, high], axis=0))
        outer = outer + dot(parts_ref[:, :128], low)
        blocks = []
        for k in range(2):
            own = outer[:, k * 128 : k * 128 + 128].reshape(8, 4, 32, 128)
            moved = swap_groups([own[:, y] for y in range(4)])
            blocks += [jnp.concatenate([moved[i][y] for y in range(8)], axis=1) for i in range(4)]
        high, low = halves(jnp.concatenate(blocks, axis=0))
        update = dot(high, both_ref[...])
        update = update[:, :128] + (update[:, 128:] + dot(low, both_ref[:, :128]))
        update = update.reshape(2, 4, 4, 8, 128)
        for k in range(2):
            for r in range(4):
                out_ref[2 * z + k, r] = update[k, :, r]


def pair_kernel(parts_ref, pair_ref, gain_ref, weight_ref, pair_out_ref, bias_ref):
    total = parts_ref[0]
    for g in range(1, 8):
        total = total + parts_ref[g]
    total = total * (1.0 / 1024.0)
    for x in range(2):
        for c in range(2):
            at = c * 8 + x * 4
            pair_out_ref[at : at + 4] = pair_ref[at : at + 4] + total[(x * 2 + c) * 4 : (x * 2 + c) * 4 + 4]
    normed = center_scale(pair_out_ref[...].reshape(128, 128)) * gain_ref[...]
    bias = dot6(weight_ref[...], normed, (((1,), (1,)), ((), ())))
    for copy in range(4):
        bias_ref[copy] = bias


def attend_kernel(own_ref, *refs):
    kept, moved, (bias_ref, out_ref, qkv_ref) = refs[:4], refs[4:6], refs[6:]
    pieces = list(kept) + [moved[k % 2].at[k // 2] for k in range(4)]
    for k in range(8):
        z, x, core = (k // 4) ^ own_ref[0], (k // 2 % 2) ^ own_ref[1], (k % 2) ^ own_ref[2]
        qkv_ref[z * 4 + x * 2 + core] = pieces[k][...]
    bias = bias_ref[...].reshape(256, 256)
    group = lane_group((256, 128))
    dot = functools.partial(jnp.dot, preferred_element_type=f32)
    across = (((1,), (1,)), ((), ()))
    dot_across = functools.partial(
        lax.dot_general, dimension_numbers=across, preferred_element_type=f32
    )

    def residues(t, n):
        return jnp.concatenate([qkv_ref[:, t, n, z].reshape(64, 128) for z in range(4)], axis=0)

    def step(n, carry):
        query = residues(0, n)
        key_high, key_low = halves(residues(1, n))
        keys = jnp.concatenate([key_high, key_high], axis=1)
        value_high, value_low = halves(residues(2, n))
        values = jnp.concatenate([value_high, value_low], axis=1)
        mixed = jnp.zeros((256, 128), f32)
        for s in range(4):
            high, low = halves(jnp.where(group == s, query, 0.0))
            scores = dot_across(jnp.concatenate([high, low], axis=1), keys)
            scores = scores + dot_across(high, key_low) + bias
            top = jnp.max(scores, axis=-1, keepdims=True)
            weights = jnp.exp(scores - top)
            total = jnp.sum(weights, axis=-1, keepdims=True)
            high, low = halves(weights)
            both = dot(high, values)
            summed = both[:, :128] + (both[:, 128:] + dot(low, value_high))
            mixed = jnp.where(group == s, summed / total, mixed)
        out_ref[:, n] = mixed.reshape(32, 8, 128)
        return carry

    lax.fori_loop(0, 4, step, 0)


def output_kernel(mixed_ref, gate_ref, rows_ref, weight_ref, out_ref):
    columns = []
    for half in range(2):
        parts = [mixed_ref[:, half * 4 + h].reshape(16, 8, 128) for h in range(4)]
        columns.append(jnp.stack(swap_groups(parts), axis=1).reshape(512, 128))
    gated = jnp.concatenate(columns, axis=1) * gate_ref[...]
    out_ref[...] = rows_ref[...] + dot3(gated, weight_ref[...])


def shape_of(*lengths):
    return jax.ShapeDtypeStruct(lengths, f32)


def call(kernel, flops, out_shape, *args, scratch=(), scalars=0):
    specs = [pl.BlockSpec(memory_space=pltpu.SMEM)] * scalars
    specs += [pl.BlockSpec(memory_space=pltpu.VMEM)] * (len(args) - scalars)
    return pl.pallas_call(
        kernel,
        in_specs=specs,
        out_shape=out_shape,
        scratch_shapes=list(scratch),
        cost_estimate=pl.CostEstimate(flops=flops, bytes_accessed=2**20, transcendentals=0),
        compiler_params=pltpu.CompilerParams(vmem_limit_bytes=24 * 2**20),
    )(*args)


def exchanged(value, axes):
    return lax.all_to_all(value, axes, 0, 0, tiled=True)


def sent_to_all(value, axes):
    count = lax.axis_size(axes)
    return exchanged(jnp.broadcast_to(value[None], (count, *value.shape)), axes)


def on_device(
    alignment,
    pair_features,
    outer_gain,
    w_outer_in,
    w_outer_out,
    pair_gain,
    w_bias,
    row_gain,
    w_project,
    w_output,
):
    rows = alignment.reshape(512, 256)
    gain = row_gain.reshape(1, 256)
    y, z, x, core = (lax.axis_index(axis) for axis in ("yl", "zl", "xl", "core"))
    own = jnp.stack([z, x, core])
    left, right = call(
        maps_kernel,
        10**9,
        (shape_of(2, 64, 128), shape_of(64, 256)),
        rows,
        w_outer_in.T * outer_gain[None],
        scratch=[pltpu.VMEM((512, 128), f32)],
    )
    moved_rows = exchanged(alignment.reshape(4, 16, 8, 256), "zh").reshape(512, 256)
    left_a = lax.dynamic_index_in_dim(left, y, 0, keepdims=False)
    left_b = lax.dynamic_index_in_dim(left, 1 - y, 0, keepdims=False)
    left_a = lax.ppermute(left_a, ("yl", "xl"), [(0, 0), (1, 2), (2, 1), (3, 3)])
    left_b = lax.ppermute(left_b, ("yl", "xl"), [(0, 1), (1, 3), (2, 0), (3, 2)])
    swap = [(0, 1), (1, 0)]
    other = lax.ppermute(right, "core", swap)
    right = jnp.where(core == 0, jnp.stack([right, other]), jnp.stack([other, right]))
    left_a, left_b, moved_rows = lax.optimization_barrier((left_a, left_b, moved_rows))
    left = jnp.where(x == y, jnp.stack([left_a, left_b]), jnp.stack([left_b, left_a]))
    left_all = sent_to_all(left, ("zh", "zl")).reshape(8, 2, 64, 128)
    other = lax.ppermute(right, "xl", swap)
    qkv = call(
        project_kernel,
        4 * 10**9,
        shape_of(2, 2, 2, 3, 4, 4, 8, 128),
        own,
        moved_rows,
        gain,
        w_project[:, :768],
        scalars=1,
    )
    other, qkv = lax.optimization_barrier((other, qkv))
    right = jnp.where(x == 0, jnp.concatenate([right, other]), jnp.concatenate([other, right]))
    other = lax.ppermute(right, "yl", swap)
    order, qkv = lax.optimization_barrier((own, qkv))
    far_core = lax.ppermute(qkv[1], "core", swap)
    far_x = lax.ppermute(qkv[0, 1], "xl", swap)
    parts = call(
        outer_kernel,
        4 * 10**9,
        shape_of(8, 4, 4, 8, 128),
        order,
        left_all,
        right,
        other,
        w_outer_out,
        scratch=[
            pltpu.VMEM((4, 256, 128), f32),
            pltpu.VMEM((1024, 128), f32),
            pltpu.VMEM((1024, 256), bf16),
            pltpu.VMEM((1024, 256), bf16),
        ],
        scalars=1,
    )
    parts, far_core = lax.optimization_barrier((parts, far_core))
    parts = exchanged(parts.reshape(32, 4, 8, 128), ("xh", "yh", "xl", "core"))
    last = lax.ppermute(far_core[1], "xl", swap)
    moved = lax.ppermute(jnp.stack([qkv[0, 0, 1], far_x[1]]), "zl", swap)
    kept = [qkv[0, 0, 0], far_core[0, 0], far_x[0], last[0]]
    sent = jnp.stack([far_core[0, 1], last[1]])
    parts, kept, sent = lax.optimization_barrier((parts, kept, sent))
    updated_pair, bias = call(
        pair_kernel,
        10**8,
        (shape_of(16, 8, 128), shape_of(4, 8, 128)),
        parts.reshape(8, 16, 8, 128),
        pair_features,
        pair_gain.reshape(1, 128),
        w_bias.T,
    )
    bias, sent = lax.optimization_barrier((bias, sent))
    pieces = kept + [moved, lax.ppermute(sent, "zl", swap)]
    bias = exchanged(bias.reshape(32, 128), RES)
    bias = bias.reshape(32, 16, 8).transpose(1, 0, 2).reshape(16, 256)
    late_gain, bias = lax.optimization_barrier((gain, bias))
    gate = call(gate_kernel, 10**9, shape_of(512, 256), rows, late_gain, w_project[:, 768:])
    bias = sent_to_all(bias, SEQ).reshape(16, 16, 256)
    bias, gate = lax.optimization_barrier((bias, gate))
    mixed = call(
        attend_kernel,
        4 * 10**9,
        shape_of(32, 4, 8, 128),
        own,
        *pieces,
        bias,
        scratch=[pltpu.VMEM((8, 3, 4, 4, 8, 128), f32)],
        scalars=1,
    )
    mixed = exchanged(mixed, RES)
    out = call(
        output_kernel,
        10**9,
        shape_of(512, 256),
        mixed.reshape(4, 8, 4, 8, 128),
        gate,
        rows,
        w_output,
    )
    return out.reshape(alignment.shape), updated_pair


def solution(mesh):
    fine = Mesh(
        mesh.devices.reshape(2, 4, 2, 4, 2, 2, 2), ("xh", "yh", "yl", "zh", "zl", "xl", "core")
    )
    tiled = P(SEQ, RES, None)
    return jax.shard_map(
        on_device,
        mesh=fine,
        in_specs=(tiled, tiled) + (P(),) * 8,
        out_specs=(tiled, tiled),
        check_vma=False,
    )
```

```python
import functools

import jax
import jax.numpy as jnp
from jax import lax
from jax.experimental import pallas as pl
from jax.experimental.pallas import tpu as pltpu
from jax.sharding import Mesh, PartitionSpec as P


f32 = jnp.float32
bf16 = jnp.bfloat16
precise = lax.Precision.HIGHEST

SEQ = ("xh", "yh", "yl")
RES = ("zh", "zl", "xl", "core")


def dot6(a, b, dims=(((1,), (0,)), ((), ()))):
    return lax.dot_general(a, b, dims, precision=precise, preferred_element_type=f32)


def halves(x):
    high = x.astype(bf16)
    low = (x - high.astype(f32)).astype(bf16)
    return high, low


def dot_parts(a, b, dims=(((1,), (0,)), ((), ()))):
    dot = functools.partial(lax.dot_general, dimension_numbers=dims, preferred_element_type=f32)
    return dot(a[0], b[0]) + (dot(a[0], b[1]) + dot(a[1], b[0]))


def dot3(a, b, dims=(((1,), (0,)), ((), ()))):
    return dot_parts(halves(a), halves(b), dims)


def center_scale(x):
    average = jnp.mean(x, axis=-1, keepdims=True)
    centered = x - average
    variance = jnp.mean(centered * centered, axis=-1, keepdims=True)
    return centered * lax.rsqrt(variance + 1e-05)


def lane_group(shape):
    return lax.broadcasted_iota(jnp.int32, shape, len(shape) - 1) // 32


def lanes_moved(x, shift):
    rows = x.reshape(-1, 128)
    return pltpu.roll(rows, shift % 128, 1).reshape(x.shape)


def swap_groups(parts):
    group = lane_group(parts[0].shape)
    low = group % 2 == 0
    x = [None] * 4
    for a in (0, 2):
        x[a] = jnp.where(low, parts[a], lanes_moved(parts[a + 1], 32))
        x[a + 1] = jnp.where(low, lanes_moved(parts[a], -32), parts[a + 1])
    first = group < 2
    y = [None] * 4
    for a in (0, 1):
        y[a] = jnp.where(first, x[a], lanes_moved(x[a + 2], 64))
        y[a + 2] = jnp.where(first, lanes_moved(x[a], 64), x[a + 2])
    return y


def maps_kernel(rows_ref, weight_ref, left_ref, right_ref, maps_ref):
    normed = center_scale(rows_ref[...])
    maps_ref[:, :64] = dot6(normed, weight_ref[...], (((1,), (1,)), ((), ())))
    count = left_ref.shape[1]
    group = lane_group((count, 128))
    for half in range(2):
        left = jnp.zeros((count, 128), f32)
        right = jnp.zeros((count, 128), f32)
        for k in range(4):
            part = maps_ref[pl.ds(half * 4 + k, count, stride=8), :]
            left = jnp.where(group == k, lanes_moved(part, 32 * k), left)
            right = jnp.where(group == k, lanes_moved(part, 32 * k - 32), right)
        left_ref[half] = left
        right_ref[:, half * 128 : half * 128 + 128] = right


def project_kernel(own_ref, rows_ref, gain_ref, weight_ref, qkv_ref):
    normed = halves(center_scale(rows_ref[...]) * gain_ref[...])
    for t in range(3):
        block = dot_parts(normed, halves(weight_ref[:, t * 256 : t * 256 + 256]))
        if t == 0:
            block = block * 32 ** (-0.5)
        for half in range(2):
            part = block[:, half * 128 : half * 128 + 128].reshape(16, 4, 8, 128)
            moved = swap_groups([part[:, s] for s in range(4)])
            for h in range(4):
                own = moved[h].reshape(4, 4, 8, 128)
                z, x, core = half ^ own_ref[0], (h // 2) ^ own_ref[1], (h % 2) ^ own_ref[2]
                for n in range(4):
                    qkv_ref[core, x, z, t, n] = own[:, n]


def gate_kernel(rows_ref, gain_ref, weight_ref, gate_ref):
    normed = center_scale(rows_ref[...]) * gain_ref[...]
    gate_ref[...] = jax.nn.sigmoid(dot3(normed, weight_ref[...]))


def weight_kernel(weight_ref, both_ref):
    for y in range(32):
        high, low = halves(weight_ref[pl.ds(y, 32, stride=32), :])
        both_ref[y * 32 : y * 32 + 32, :128] = high
        both_ref[y * 32 : y * 32 + 32, 128:] = low


def outer_kernel(
    order_ref, left_ref, own_ref, other_ref, both_ref, out_ref, turned_ref, rows_ref, parts_ref
):
    for r in range(4):
        both = jnp.concatenate([own_ref[r], other_ref[r]], axis=0)
        turned_ref[r] = both.T
    for y in range(32):
        for r in range(4):
            rows_ref[(y * 4 + r) * 8 : (y * 4 + r) * 8 + 8, :] = turned_ref[r, pl.ds(y, 8, stride=32), :]
    high, low = halves(rows_ref[...])
    parts_ref[:, :128] = high
    parts_ref[:, 128:] = low
    dot = functools.partial(jnp.dot, preferred_element_type=f32)

    for z in range(4):
        left = jnp.concatenate(
            [
                jnp.concatenate([left_ref[2 * z + k, 0], left_ref[2 * z + k, 1]], axis=0)
                for k in range(2)
            ],
            axis=1,
        )
        high, low = halves(left)
        outer = dot(parts_ref[...], jnp.concatenate([high, high], axis=0))
        outer = outer + dot(parts_ref[:, :128], low)
        blocks = []
        for k in range(2):
            own = outer[:, k * 128 : k * 128 + 128].reshape(8, 4, 32, 128)
            moved = swap_groups([own[:, y] for y in range(4)])
            blocks += [jnp.concatenate([moved[i][y] for y in range(8)], axis=1) for i in range(4)]
        high, low = halves(jnp.concatenate(blocks, axis=0))
        update = dot(high, both_ref[...])
        update = update[:, :128] + (update[:, 128:] + dot(low, both_ref[:, :128]))
        update = update.reshape(2, 4, 4, 8, 128)
        for k in range(2):
            for r in range(4):
                out_ref[2 * z + k, r] = update[k, :, r]


def pair_kernel(parts_ref, pair_ref, gain_ref, weight_ref, pair_out_ref, bias_ref):
    total = parts_ref[0]
    for g in range(1, 8):
        total = total + parts_ref[g]
    total = total * (1.0 / 1024.0)
    for x in range(2):
        for c in range(2):
            at = c * 8 + x * 4
            pair_out_ref[at : at + 4] = pair_ref[at : at + 4] + total[(x * 2 + c) * 4 : (x * 2 + c) * 4 + 4]
    normed = center_scale(pair_out_ref[...].reshape(128, 128)) * gain_ref[...]
    bias = dot6(weight_ref[...], normed, (((1,), (1,)), ((), ())))
    for copy in range(4):
        bias_ref[copy] = bias


def attend_kernel(own_ref, *refs):
    kept, moved, (bias_ref, out_ref, qkv_ref) = refs[:4], refs[4:6], refs[6:]
    pieces = list(kept) + [moved[k % 2].at[k // 2] for k in range(4)]
    for k in range(8):
        z, x, core = (k // 4) ^ own_ref[0], (k // 2 % 2) ^ own_ref[1], (k % 2) ^ own_ref[2]
        qkv_ref[z * 4 + x * 2 + core] = pieces[k][...]
    bias = bias_ref[...].reshape(256, 256)
    group = lane_group((256, 128))
    dot = functools.partial(jnp.dot, preferred_element_type=f32)
    across = (((1,), (1,)), ((), ()))
    dot_across = functools.partial(
        lax.dot_general, dimension_numbers=across, preferred_element_type=f32
    )

    def residues(t, n):
        return jnp.concatenate([qkv_ref[:, t, n, z].reshape(64, 128) for z in range(4)], axis=0)

    def step(n, carry):
        query = residues(0, n)
        key_high, key_low = halves(residues(1, n))
        keys = jnp.concatenate([key_high, key_high], axis=1)
        value_high, value_low = halves(residues(2, n))
        values = jnp.concatenate([value_high, value_low], axis=1)
        mixed = jnp.zeros((256, 128), f32)
        for s in range(4):
            high, low = halves(jnp.where(group == s, query, 0.0))
            scores = dot_across(jnp.concatenate([high, low], axis=1), keys)
            scores = scores + dot_across(high, key_low) + bias
            top = jnp.max(scores, axis=-1, keepdims=True)
            weights = jnp.exp(scores - top)
            total = jnp.sum(weights, axis=-1, keepdims=True)
            high, low = halves(weights)
            both = dot(high, values)
            summed = both[:, :128] + (both[:, 128:] + dot(low, value_high))
            mixed = jnp.where(group == s, summed / total, mixed)
        out_ref[:, n] = mixed.reshape(32, 8, 128)
        return carry

    lax.fori_loop(0, 4, step, 0)


def output_kernel(mixed_ref, gate_ref, rows_ref, weight_ref, out_ref):
    columns = []
    for half in range(2):
        parts = [mixed_ref[:, half * 4 + h].reshape(16, 8, 128) for h in range(4)]
        columns.append(jnp.stack(swap_groups(parts), axis=1).reshape(512, 128))
    gated = jnp.concatenate(columns, axis=1) * gate_ref[...]
    out_ref[...] = rows_ref[...] + dot3(gated, weight_ref[...])


def shape_of(*lengths):
    return jax.ShapeDtypeStruct(lengths, f32)


def call(kernel, flops, out_shape, *args, scratch=(), scalars=0):
    specs = [pl.BlockSpec(memory_space=pltpu.SMEM)] * scalars
    specs += [pl.BlockSpec(memory_space=pltpu.VMEM)] * (len(args) - scalars)
    return pl.pallas_call(
        kernel,
        in_specs=specs,
        out_shape=out_shape,
        scratch_shapes=list(scratch),
        cost_estimate=pl.CostEstimate(flops=flops, bytes_accessed=2**20, transcendentals=0),
        compiler_params=pltpu.CompilerParams(vmem_limit_bytes=24 * 2**20),
    )(*args)


def exchanged(value, axes):
    return lax.all_to_all(value, axes, 0, 0, tiled=True)


def sent_to_all(value, axes):
    count = lax.axis_size(axes)
    return exchanged(jnp.broadcast_to(value[None], (count, *value.shape)), axes)


def on_device(
    alignment,
    pair_features,
    outer_gain,
    w_outer_in,
    w_outer_out,
    pair_gain,
    w_bias,
    row_gain,
    w_project,
    w_output,
):
    rows = alignment.reshape(512, 256)
    gain = row_gain.reshape(1, 256)
    y, z, x, core = (lax.axis_index(axis) for axis in ("yl", "zl", "xl", "core"))
    own = jnp.stack([z, x, core])
    left, right = call(
        maps_kernel,
        10**9,
        (shape_of(2, 64, 128), shape_of(64, 256)),
        rows,
        w_outer_in.T * outer_gain[None],
        scratch=[pltpu.VMEM((512, 128), f32)],
    )
    moved_rows = exchanged(alignment.reshape(4, 16, 8, 256), "zh").reshape(512, 256)
    left_a = lax.dynamic_index_in_dim(left, y, 0, keepdims=False)
    left_b = lax.dynamic_index_in_dim(left, 1 - y, 0, keepdims=False)
    left_a = lax.ppermute(left_a, ("yl", "xl"), [(0, 0), (1, 2), (2, 1), (3, 3)])
    left_b = lax.ppermute(left_b, ("yl", "xl"), [(0, 1), (1, 3), (2, 0), (3, 2)])
    swap = [(0, 1), (1, 0)]
    other = lax.ppermute(right, "core", swap)
    right = jnp.where(core == 0, jnp.stack([right, other]), jnp.stack([other, right]))
    left_a, left_b, moved_rows = lax.optimization_barrier((left_a, left_b, moved_rows))
    left = jnp.where(x == y, jnp.stack([left_a, left_b]), jnp.stack([left_b, left_a]))
    left_all = sent_to_all(left, ("zh", "zl")).reshape(8, 2, 64, 128)
    other = lax.ppermute(right, "xl", swap)
    qkv = call(
        project_kernel,
        4 * 10**9,
        shape_of(2, 2, 2, 3, 4, 4, 8, 128),
        own,
        moved_rows,
        gain,
        w_project[:, :768],
        scalars=1,
    )
    other, qkv = lax.optimization_barrier((other, qkv))
    right = jnp.where(x == 0, jnp.concatenate([right, other]), jnp.concatenate([other, right]))
    other = lax.ppermute(right, "yl", swap)
    late_weight, qkv = lax.optimization_barrier((w_outer_out, qkv))
    both = call(weight_kernel, 10**6, jax.ShapeDtypeStruct((1024, 256), bf16), late_weight)
    order, qkv = lax.optimization_barrier((own, qkv))
    far_core = lax.ppermute(qkv[1], "core", swap)
    far_x = lax.ppermute(qkv[0, 1], "xl", swap)
    parts = call(
        outer_kernel,
        4 * 10**9,
        shape_of(8, 4, 4, 8, 128),
        order,
        left_all,
        right,
        other,
        both,
        scratch=[
            pltpu.VMEM((4, 256, 128), f32),
            pltpu.VMEM((1024, 128), f32),
            pltpu.VMEM((1024, 256), bf16),
        ],
        scalars=1,
    )
    parts, far_core = lax.optimization_barrier((parts, far_core))
    parts = exchanged(parts.reshape(32, 4, 8, 128), ("xh", "yh", "xl", "core"))
    last = lax.ppermute(far_core[1], "xl", swap)
    moved = lax.ppermute(jnp.stack([qkv[0, 0, 1], far_x[1]]), "zl", swap)
    kept = [qkv[0, 0, 0], far_core[0, 0], far_x[0], last[0]]
    sent = jnp.stack([far_core[0, 1], last[1]])
    parts, kept, sent = lax.optimization_barrier((parts, kept, sent))
    updated_pair, bias = call(
        pair_kernel,
        10**8,
        (shape_of(16, 8, 128), shape_of(4, 8, 128)),
        parts.reshape(8, 16, 8, 128),
        pair_features,
        pair_gain.reshape(1, 128),
        w_bias.T,
    )
    bias, sent = lax.optimization_barrier((bias, sent))
    pieces = kept + [moved, lax.ppermute(sent, "zl", swap)]
    bias = exchanged(bias.reshape(32, 128), RES)
    bias = bias.reshape(32, 16, 8).transpose(1, 0, 2).reshape(16, 256)
    late_gain, bias = lax.optimization_barrier((gain, bias))
    gate = call(gate_kernel, 10**9, shape_of(512, 256), rows, late_gain, w_project[:, 768:])
    bias = sent_to_all(bias, SEQ).reshape(16, 16, 256)
    bias, gate = lax.optimization_barrier((bias, gate))
    mixed = call(
        attend_kernel,
        4 * 10**9,
        shape_of(32, 4, 8, 128),
        own,
        *pieces,
        bias,
        scratch=[pltpu.VMEM((8, 3, 4, 4, 8, 128), f32)],
        scalars=1,
    )
    mixed = exchanged(mixed, RES)
    out = call(
        output_kernel,
        10**9,
        shape_of(512, 256),
        mixed.reshape(4, 8, 4, 8, 128),
        gate,
        rows,
        w_output,
    )
    return out.reshape(alignment.shape), updated_pair


def solution(mesh):
    fine = Mesh(
        mesh.devices.reshape(2, 4, 2, 4, 2, 2, 2), ("xh", "yh", "yl", "zh", "zl", "xl", "core")
    )
    tiled = P(SEQ, RES, None)
    return jax.shard_map(
        on_device,
        mesh=fine,
        in_specs=(tiled, tiled) + (P(),) * 8,
        out_specs=(tiled, tiled),
        check_vma=False,
    )
```
